32 devices in a mesh: batch: 8 (over z, y), mp: 4 (over x, core).
Axes of the slice: x: 2, y: 2, z: 4, core: 2. Of those that a mesh axis runs over, the one named last changes fastest.
Arguments:
- init_state: float32 [4096, 256], P(('batch', 'mp')), may hold values from -6 to 6
- brownian: bfloat16 [32, 4096, 256], P(None, ('batch', 'mp')), may hold values from -6 to 6
- step_size: float32 [4096], P(('batch', 'mp')), may hold values from 0.02 to 0.1
- lengths: int32 [4096], P(('batch', 'mp')), may hold values from 1 to 32, as said below
- obs_steps: int32 [4096, 8], P(('batch', 'mp')), may hold values from 1 to 32, as said below
- observed: bfloat16 [4096, 8, 128], P(('batch', 'mp')), may hold values from -6 to 6
- w_in: bfloat16 [256, 1024], P(None, 'mp'), may hold values from -0.375 to 0.375
- b_in: bfloat16 [1024], P('mp'), may hold values from -3 to 3
- w_out: bfloat16 [1024, 256], P('mp'), may hold values from -0.1875 to 0.1875
- b_out: float32 [256], replicated, may hold values from -4 to 4
- decoder: bfloat16 [256, 128], replicated, may hold values from -0.375 to 0.375
- prior_rate: float32 [256], replicated, may hold values from 0.1 to 2
- diffusion: float32 [256], replicated, may hold values from 0.7 to 1.4
Outputs:
- elbo_series: float32 [4096], P(('batch', 'mp'))
- scores: float32 [2], replicated
- grad_w_in: float32 [256, 1024], P(None, 'mp')
- grad_b_in: float32 [1024], P('mp')
- grad_w_out: float32 [1024, 256], P('mp')
- grad_b_out: float32 [256], replicated
- grad_decoder: float32 [256, 128], replicated
- grad_init: float32 [4096, 256], P(('batch', 'mp'))
The draws below stay inside these ranges and needn't reach their ends.
Inputs may be any that keep to these rules, and one draw needn't show every extreme that they name: `lengths`: some series has 32 live steps in every draw. obs_steps[i, j] is at most lengths[i].
All inputs are finite; a program needn't handle non-finite values.
Results may differ from the reference program's by a relative error of at most 0.0019.
Values may be sent and summed in bfloat16 or wider, within the bound.
A program may use at most 64 MiB of HBM per device.

```python
import math
import jax
import jax.numpy as jnp
from jax import lax

L = 256
H = 1024
P_SIZE = 128
OBS = 8
S_STEPS = 32
ROWS_DEV = 128
SERIES = 4096


def length_table(key):
    block_count = SERIES // ROWS_DEV
    key_ceiling, key_choose, key_length, key_place = jax.random.split(jax.random.fold_in(key, 11), 4)
    ceilings = jax.random.randint(key_ceiling, (block_count,), S_STEPS // 4, S_STEPS + 1)
    chosen = jax.random.randint(key_choose, (), 0, block_count)
    ceilings = jnp.where(jnp.arange(block_count) == chosen, S_STEPS, ceilings)
    per_row = jnp.repeat(ceilings, ROWS_DEV, total_repeat_length=SERIES)
    drawn = jax.random.randint(key_length, (SERIES,), 1, per_row + 1)
    places = jax.random.randint(key_place, (block_count,), 0, ROWS_DEV)
    topmost = jnp.arange(SERIES) % ROWS_DEV == jnp.repeat(places, ROWS_DEV, total_repeat_length=SERIES)
    return jnp.where(topmost, per_row, drawn).astype(jnp.int32)


def draw_lengths(key, part):
    return length_table(key)


def draw_obs_steps(key, part):
    table = length_table(key)
    picks = jax.random.randint(jax.random.fold_in(key, 23), (SERIES, OBS), 1, table[:, None] + 1)
    return picks.astype(jnp.int32)


def levels(rng, shape, cuts, smallest, top_value):
    level, own = 1.0, jax.random.fold_in(rng, 6)
    for axis_at, blocks in cuts:
        steps = jnp.exp(jax.random.uniform(jax.random.fold_in(own, axis_at), (blocks,), jnp.float32, smallest / len(cuts), top_value / len(cuts)))
        level = level * jnp.repeat(steps, shape[axis_at] // blocks).reshape([-1 if axis == axis_at else 1 for axis in range(len(shape))])
    return level


def gaussian(own_key, extent, spread, bound, cuts=(), kind=jnp.bfloat16):
    gain = levels(own_key, extent, cuts, -0.22, 0.18) if cuts else 1.0
    values = jax.random.normal(own_key, extent, jnp.float32) * spread * gain
    return jnp.minimum(jnp.maximum(values, -bound), bound).astype(kind)


def setup_inputs(seed: int = 0) -> dict:
    key_list = jax.random.split(jax.random.key(seed), 14)
    init_state = gaussian(key_list[0], (SERIES, L), 1.0, 6.0, ((0, 32),), jnp.float32)
    brownian = gaussian(key_list[1], (S_STEPS, SERIES, L), 1.0, 6.0, ((1, 32),))
    step_size = jnp.clip(jnp.exp(math.log(0.1) - 1.609438 * jax.random.uniform(key_list[2], (SERIES,), jnp.float32) ** levels(key_list[2], (SERIES,), ((0, 32),), -0.2, 0.2)), 0.02, 0.1)
    lengths = draw_lengths(jax.random.fold_in(key_list[13], 71), 0)
    obs_steps = draw_obs_steps(jax.random.fold_in(key_list[13], 71), 0)
    observed = gaussian(key_list[5], (SERIES, OBS, P_SIZE), 1.0, 6.0, ((0, 32),))
    w_in = gaussian(key_list[6], (L, H), L ** -0.5, 0.375, ((1, 4),))
    b_in = gaussian(key_list[7], (H,), 0.5, 3.0, ((0, 4),))
    w_out = gaussian(key_list[8], (H, L), H ** -0.5, 0.1875, ((0, 4),))
    b_out = gaussian(key_list[9], (L,), 1.0, 4.0, (), jnp.float32)
    decoder = gaussian(key_list[10], (L, P_SIZE), L ** -0.5, 0.375)
    prior_rate = jnp.clip(jnp.exp(jax.random.uniform(key_list[11], (L,), jnp.float32, math.log(0.1), math.log(2.0))), 0.1, 2.0)
    diffusion = jnp.clip(jax.random.uniform(key_list[12], (L,), jnp.float32, 0.7, 1.4), 0.7, 1.4)
    return dict(init_state=init_state, brownian=brownian, step_size=step_size, lengths=lengths, obs_steps=obs_steps, observed=observed, w_in=w_in, b_in=b_in, w_out=w_out, b_out=b_out, decoder=decoder, prior_rate=prior_rate, diffusion=diffusion)


def block_terms(block_init, block_noise, block_step, block_lengths, block_obs, block_observed, w_in, b_in, w_out, b_out, decoder, prior_rate, diffusion):
    row_count = block_init.shape[0]
    num_steps = block_noise.shape[0]
    live_mask = (jnp.arange(num_steps, dtype=jnp.int32)[:, None] < block_lengths[None, :]).astype(jnp.float32)
    step_col = block_step[:, None]
    root_col = jnp.sqrt(block_step)[:, None]
    bias_in = b_in.astype(jnp.float32)

    def forward(loop_state, inputs):
        current, kl_sum = loop_state
        increment, live_now = inputs
        activity = jnp.tanh(jnp.dot(current.astype(jnp.bfloat16), w_in, preferred_element_type=jnp.float32) + bias_in).astype(jnp.bfloat16)
        drift_now = jnp.dot(activity, w_out, preferred_element_type=jnp.float32) + b_out
        residual = (drift_now + prior_rate * current) / diffusion
        kl_sum = kl_sum + live_now * 0.5 * block_step * lax.optimization_barrier(jnp.sum(residual * residual, axis=1))
        following = current + live_now[:, None] * (step_col * drift_now + diffusion * root_col * increment.astype(jnp.float32))
        return ((following, kl_sum), (current, activity, residual))
    (last_state, kl_total), (visited, activities, residuals) = lax.scan(forward, (block_init, jnp.zeros((row_count,), jnp.float32)), (block_noise, live_mask))
    trajectory = jnp.concatenate([visited, last_state[None]], axis=0)
    picked = trajectory[block_obs, jnp.arange(row_count, dtype=jnp.int32)[:, None]]
    picked_round = picked.astype(jnp.bfloat16).reshape(-1, picked.shape[2])
    flat_obs = block_observed.reshape(-1, block_observed.shape[2]).astype(jnp.float32)
    misfit = jnp.dot(picked_round, decoder, preferred_element_type=jnp.float32) - flat_obs
    loglik = -0.5 * lax.optimization_barrier(jnp.sum((misfit * misfit).reshape(row_count, -1), axis=1))
    misfit_round = misfit.astype(jnp.bfloat16)
    decoder_grad = jnp.dot(picked_round.T, misfit_round, preferred_element_type=jnp.float32)
    misfit_back = jnp.dot(misfit_round, decoder.T, preferred_element_type=jnp.float32).reshape(row_count, block_obs.shape[1], -1)
    onehot = (block_obs[:, :, None] == jnp.arange(num_steps + 1, dtype=jnp.int32)[None, None, :]).astype(jnp.float32)
    obs_back = jnp.einsum('bjs,bjl->sbl', onehot, misfit_back, precision=lax.Precision.HIGHEST)

    def backward(loop_state, inputs):
        cotangent, sum_w_in, sum_b_in, sum_w_out, sum_b_out = loop_state
        current, activity, residual, live_now, obs_here = inputs
        factor = (live_now * block_step)[:, None]
        scaled = residual / diffusion
        update = factor * (cotangent + scaled)
        update_round = update.astype(jnp.bfloat16)
        activity_value = activity.astype(jnp.float32)
        pre_grad = jnp.dot(update_round, w_out.T, preferred_element_type=jnp.float32) * (1.0 - activity_value * activity_value)
        pre_round = pre_grad.astype(jnp.bfloat16)
        cotangent = cotangent + factor * prior_rate * scaled + jnp.dot(pre_round, w_in.T, preferred_element_type=jnp.float32) + obs_here
        sum_w_in = sum_w_in + jnp.dot(current.astype(jnp.bfloat16).T, pre_round, preferred_element_type=jnp.float32)
        sum_b_in = sum_b_in + lax.optimization_barrier(jnp.sum(pre_grad, axis=0))
        sum_w_out = sum_w_out + jnp.dot(activity.T, update_round, preferred_element_type=jnp.float32)
        sum_b_out = sum_b_out + lax.optimization_barrier(jnp.sum(update, axis=0))
        return ((cotangent, sum_w_in, sum_b_in, sum_w_out, sum_b_out), None)
    start_back = (obs_back[num_steps], jnp.zeros(w_in.shape, jnp.float32), jnp.zeros((w_in.shape[1],), jnp.float32), jnp.zeros(w_out.shape, jnp.float32), jnp.zeros((w_out.shape[1],), jnp.float32))
    (cotangent, sum_w_in, sum_b_in, sum_w_out, sum_b_out), _ = lax.scan(backward, start_back, (visited, activities, residuals, live_mask, obs_back[:num_steps]), reverse=True)
    divisor = (L * block_lengths + P_SIZE * OBS).astype(jnp.float32)
    elbo_rows = (loglik - kl_total) / divisor
    return (elbo_rows, cotangent, jnp.sum(loglik), jnp.sum(kl_total), sum_w_in, sum_b_in, sum_w_out, sum_b_out, decoder_grad)

def reference(init_state, brownian, step_size, lengths, obs_steps, observed, w_in, b_in, w_out, b_out, decoder, prior_rate, diffusion):
    block_count = SERIES // ROWS_DEV
    blocked = (init_state.reshape(block_count, ROWS_DEV, L), jnp.transpose(brownian.reshape(S_STEPS, block_count, ROWS_DEV, L), (1, 0, 2, 3)), step_size.reshape(block_count, ROWS_DEV), lengths.reshape(block_count, ROWS_DEV), obs_steps.reshape(block_count, ROWS_DEV, OBS), observed.reshape(block_count, ROWS_DEV, OBS, P_SIZE))
    zero_totals = (jnp.zeros((L, H), jnp.float32), jnp.zeros((H,), jnp.float32), jnp.zeros((H, L), jnp.float32), jnp.zeros((L,), jnp.float32), jnp.zeros((L, P_SIZE), jnp.float32), jnp.zeros((), jnp.float32), jnp.zeros((), jnp.float32))

    def visit(totals, pieces):
        outcome = block_terms(pieces[0], pieces[1], pieces[2], pieces[3], pieces[4], pieces[5], w_in, b_in, w_out, b_out, decoder, prior_rate, diffusion)
        elbo_rows, init_grad, loglik_sum, kl_sum, sum_w_in, sum_b_in, sum_w_out, sum_b_out, decoder_grad = outcome
        fresh = (sum_w_in, sum_b_in, sum_w_out, sum_b_out, decoder_grad, loglik_sum, kl_sum)
        totals = tuple((first + second for first, second in zip(totals, fresh)))
        return (totals, (elbo_rows, init_grad))
    totals, (elbo_rows, init_grads) = lax.scan(visit, zero_totals, blocked)
    elbo_series = elbo_rows.reshape(SERIES)
    grad_init = init_grads.reshape(SERIES, L)
    scores = jnp.stack([totals[5] / SERIES, totals[6] / SERIES])
    return (elbo_series, scores, totals[0] / SERIES, totals[1] / SERIES, totals[2] / SERIES, totals[3] / SERIES, totals[4] / SERIES, grad_init)
```

```python
import jax
import jax.numpy as jnp
from jax import lax
from jax.experimental import pallas as pl
from jax.experimental.pallas import tpu as pltpu
from jax.sharding import PartitionSpec as P

F32 = jnp.float32
BF16 = jnp.bfloat16
NT = (((1,), (1,)), ((), ()))
UNROLL_F = 2
UNROLL_B = 2


def dot(a, b):
    return jnp.dot(a, b, preferred_element_type=F32)


def dot_nt(a, b):
    return lax.dot_general(a, b, NT, preferred_element_type=F32)


def fold(value):
    return value.reshape(-1, 8, value.shape[1]).sum(axis=0)


def core_kernel(
    init_ref,
    noise_ref,
    step_ref,
    length_ref,
    obs_ref,
    seen_ref,
    w_in_ref,
    b_in_ref,
    w_out_ref,
    b_out_ref,
    dec_ref,
    rate_ref,
    diff_ref,
    elbo_ref,
    grads_ref,
    cot_ref,
    x_ref,
    xt_ref,
    ut_ref,
    act_ref,
    pre_ref,
    scaled_ref,
    pick_ref,
    obs_wide_ref,
    dt_ref,
    root_ref,
    len_ref,
    state_ref,
    kl_ref,
    sum_b_in_ref,
    sum_b_out_ref,
    miss_ref,
    target_ref,
    w_in_t_ref,
    w_out_t_ref,
    dec_t_ref,
    w_in_wide_ref,
    bias_ref,
):
    rows, width = init_ref.shape
    steps = noise_ref.shape[0]
    seen_count = obs_ref.shape[0]
    seen_width = dec_ref.shape[1]
    chunks = w_in_ref.shape[0]

    def column(row):
        return jnp.broadcast_to(row, (rows, rows)).T

    for n in range(chunks):
        w_in_wide_ref[:, n * width : (n + 1) * width] = w_in_ref[n]
        bias_ref[:, n * width : (n + 1) * width] = b_in_ref[n, :1, :]
    dt_ref[...] = column(step_ref[...])
    root_ref[...] = jnp.sqrt(dt_ref[...])
    len_ref[...] = column(length_ref[...])
    for j in range(seen_count):
        obs_wide_ref[j] = column(obs_ref[j : j + 1, :])
    target_ref[...] = seen_ref[...].astype(F32).reshape(target_ref.shape)
    pick_ref[...] = jnp.zeros_like(pick_ref)
    kl_ref[...] = jnp.zeros_like(kl_ref)
    sum_b_in_ref[...] = jnp.zeros_like(sum_b_in_ref)
    sum_b_out_ref[...] = jnp.zeros_like(sum_b_out_ref)
    state_ref[...] = init_ref[...]
    x_ref[0] = init_ref[...].astype(BF16)

    def both(value):
        return jnp.concatenate([value] * (width // rows), axis=1)

    def pick(index, seen):
        for j in range(seen_count):
            pick_ref[j] = jnp.where(obs_wide_ref[j] == index, seen, pick_ref[j])

    def paired(values):
        while len(values) > 2:
            values = [values[i] + values[i + 2] for i in (0, 1)] + values[4:]
        return values[0] + values[1]

    def forward(k, carry):
        x = x_ref[k]
        raw = dot(x, w_in_wide_ref[...])
        seen = dot(x, dec_ref[...])
        act = jnp.tanh(raw + bias_ref[...]).astype(BF16)
        act_ref[pl.ds(k * rows, rows), :] = act
        drift = dot(act, w_out_ref[...].reshape(chunks * width, width)) + b_out_ref[...]
        state = state_ref[...]
        inv = 1.0 / diff_ref[...]
        live = k < len_ref[...]
        factor = both(jnp.where(live, dt_ref[...], 0.0))
        root = both(jnp.where(live, root_ref[...], 0.0))
        following = state + (
            factor * drift + diff_ref[...] * root * noise_ref[k].astype(F32)
        )
        state_ref[...] = following
        x_ref[k + 1] = following.astype(BF16)
        residual = (drift + rate_ref[...] * state) * inv
        kl_ref[...] += factor * residual * residual
        scaled_ref[k] = residual * inv
        xt_ref[:, pl.ds(pl.multiple_of(k * rows, rows), rows)] = x.T
        pick(k, seen)
        return carry

    lax.fori_loop(0, steps, forward, 0, unroll=UNROLL_F)
    pick(steps, dot(x_ref[steps], dec_ref[...]))
    for n in range(chunks):
        w_in_t_ref[n * width : (n + 1) * width, :] = w_in_ref[n].T
        w_out_t_ref[:, n * width : (n + 1) * width] = w_out_ref[n].T
    dec_t = dec_ref[...].T
    dec_t_ref[:seen_width, :] = dec_t
    dec_t_ref[seen_width:, :] = dec_t

    square = jnp.zeros((rows, seen_width), F32)
    for j in range(seen_count):
        misfit = pick_ref[j] - target_ref[pl.ds(j, rows, stride=seen_count), :]
        square = square + misfit * misfit
        pick_ref[j] = misfit.astype(BF16).astype(F32)
    loglik = -0.5 * jnp.sum(square.T, axis=0, keepdims=True)
    kl_half = kl_ref[:, :rows]
    for part in range(1, width // rows):
        kl_half = kl_half + kl_ref[:, part * rows : (part + 1) * rows]
    kl_row = 0.5 * jnp.sum(kl_half.T, axis=0, keepdims=True)
    divisor = (width * length_ref[...] + seen_width * seen_count).astype(F32)
    elbo_ref[...] = (loglik - kl_row) / divisor

    def obs_back(index):
        total = jnp.zeros((rows, seen_width), F32)
        for j in range(seen_count):
            total = total + jnp.where(obs_wide_ref[j] == index, pick_ref[j], 0.0)
        high = total.astype(BF16)
        low = (total - high.astype(F32)).astype(BF16)
        wide = jnp.concatenate([high, low], axis=1)
        miss_ref[pl.ds(pl.multiple_of(index * rows, rows), rows), :] = wide
        return dot(wide, dec_t_ref[...])

    cot_ref[...] = obs_back(steps)

    def backward(index, carry):
        k = steps - 1 - index
        cot = cot_ref[...]
        scaled = scaled_ref[k]
        factor = both(jnp.where(k < len_ref[...], dt_ref[...], 0.0))
        update = factor * (cot + scaled)
        rounded = update.astype(BF16)
        raw = dot(rounded, w_out_t_ref[...])
        seen_back = obs_back(k)
        act = act_ref[pl.ds(k * rows, rows), :].astype(F32)
        pre = raw * (1.0 - act * act)
        pre_round = pre.astype(BF16)
        pre_ref[pl.ds(k * rows, rows), :] = pre_round
        sum_b_in_ref[...] += fold(pre)
        base = cot + factor * rate_ref[...] * scaled + seen_back
        cot_ref[...] = dot(pre_round, w_in_t_ref[...]) + base
        ut_ref[:, pl.ds(pl.multiple_of(k * rows, rows), rows)] = rounded.T
        sum_b_out_ref[...] += fold(update)
        return carry

    lax.fori_loop(0, steps, backward, 0, unroll=UNROLL_B)

    for n in range(chunks):
        part = pl.ds(n * width, width)
        grads_ref[n, :width, :] = dot(xt_ref[...], pre_ref[:, part])
        grads_ref[n, width : 2 * width, :] = dot(ut_ref[...], act_ref[:, part]).T
    dec_grad = dot(xt_ref[:, rows:], miss_ref[rows : steps * rows, :])
    last = lax.dot_general(
        x_ref[steps],
        miss_ref[steps * rows :, :],
        (((0,), (0,)), ((), ())),
        preferred_element_type=F32,
    )
    dec_grad = dec_grad + last
    dec_grad = dec_grad[:, :seen_width] + dec_grad[:, seen_width:]
    lanes = width // seen_width
    share = width // chunks
    tail = 2 * width
    line = tail + share // lanes
    for n in range(chunks):
        pieces = [
            dec_grad[n * share + m * share // lanes : n * share + (m + 1) * share // lanes, :]
            for m in range(lanes)
        ]
        grads_ref[n, tail:line, :] = jnp.concatenate(pieces, axis=1)
        grads_ref[n, line:, :] = jnp.zeros((grads_ref.shape[1] - line, width), F32)
        grads_ref[n, line : line + 1, :] = jnp.sum(sum_b_in_ref[:, n * width : (n + 1) * width], axis=0, keepdims=True)
        grads_ref[n, line + 1 : line + 2, :] = jnp.sum(
            sum_b_out_ref[...], axis=0, keepdims=True
        )
        grads_ref[n, line + 2 : line + 3, :rows] = loglik
        grads_ref[n, line + 2 : line + 3, rows : 2 * rows] = kl_row


def core(grad_rows, init, noise, step, length, obs, seen, w_in, b_in, w_out, b_out, dec, rate, diff):
    rows, width = init.shape
    steps = noise.shape[0]
    seen_count, seen_width = seen.shape[1], dec.shape[1]
    chunks = w_in.shape[0]
    vmem = pl.BlockSpec(memory_space=pltpu.VMEM)
    out = [
        jax.ShapeDtypeStruct((1, rows), F32),
        jax.ShapeDtypeStruct((chunks, grad_rows, width), F32),
        jax.ShapeDtypeStruct((rows, width), F32),
    ]
    resident = (6, 7, 8)
    operands = (init, noise, step, length, obs, seen, w_in, b_in, w_out, b_out, dec, rate, diff)
    loaded = [i for i in range(len(operands)) if i not in resident]
    specs = [
        vmem if i in resident else pl.BlockSpec(memory_space=pltpu.HBM)
        for i in range(len(operands))
    ]

    def body(*refs):
        refs = list(refs)
        sems = refs.pop()
        spaces = [refs.pop() for _ in loaded][::-1]
        copies = []
        for at, (i, space) in enumerate(zip(loaded, spaces)):
            copy = pltpu.make_async_copy(refs[i], space, sems.at[at])
            copy.start()
            copies.append(copy)
            refs[i] = space
        for copy in copies:
            copy.wait()
        core_kernel(*refs)

    scratch = [
        pltpu.VMEM((steps + 1, rows, width), BF16),
        pltpu.VMEM((width, steps * rows), BF16),
        pltpu.VMEM((width, steps * rows), BF16),
        pltpu.VMEM((steps * rows, chunks * width), BF16),
        pltpu.VMEM((steps * rows, chunks * width), BF16),
        pltpu.VMEM((steps, rows, width), F32),
        pltpu.VMEM((seen_count, rows, seen_width), F32),
        pltpu.VMEM((seen_count, rows, rows), jnp.int32),
        pltpu.VMEM((rows, rows), F32),
        pltpu.VMEM((rows, rows), F32),
        pltpu.VMEM((rows, rows), jnp.int32),
        pltpu.VMEM((rows, width), F32),
        pltpu.VMEM((rows, width), F32),
        pltpu.VMEM((8, chunks * width), F32),
        pltpu.VMEM((8, width), F32),
        pltpu.VMEM(((steps + 1) * rows, 2 * seen_width), BF16),
        pltpu.VMEM((rows * seen_count, seen_width), F32),
        pltpu.VMEM((chunks * width, width), BF16),
        pltpu.VMEM((width, chunks * width), BF16),
        pltpu.VMEM((2 * seen_width, width), BF16),
        pltpu.VMEM((width, chunks * width), BF16),
        pltpu.VMEM((1, chunks * width), F32),
    ]
    scratch += [pltpu.VMEM(operands[i].shape, operands[i].dtype) for i in loaded]
    scratch += [pltpu.SemaphoreType.DMA((len(loaded),))]
    return pl.pallas_call(
        body,
        out_shape=out,
        in_specs=specs,
        out_specs=[vmem] * 3,
        scratch_shapes=scratch,
        compiler_params=pltpu.CompilerParams(vmem_limit_bytes=60 * 1024 * 1024),
        cost_estimate=pl.CostEstimate(
            flops=12 * steps * rows * width * width * chunks,
            bytes_accessed=8 << 20,
            transcendentals=steps * rows * width * chunks,
        ),
        name="sde",
    )(*operands)


def send(source, target, send_sem, recv_sem, peer):
    return pltpu.make_async_remote_copy(
        src_ref=source,
        dst_ref=target,
        send_sem=send_sem,
        recv_sem=recv_sem,
        device_id=peer,
        device_id_type=pl.DeviceIdType.MESH,
    )


def greet(peers):
    barrier = pltpu.get_barrier_semaphore()
    for peer in peers:
        pl.semaphore_signal(barrier, inc=1, device_id=peer, device_id_type=pl.DeviceIdType.MESH)
    pl.semaphore_wait(barrier, len(peers))


def mp_places():
    mine = lax.axis_index("mp")
    chip, unit = mine // 2, mine % 2
    sibling = chip * 2 + (1 - unit)
    across = (1 - chip) * 2 + unit
    diagonal = (1 - chip) * 2 + (1 - unit)
    return mine, sibling, across, diagonal


def gather_kernel(w_in_ref, w_out_ref, b_in_ref, all_in_ref, all_out_ref, all_b_ref, bias_ref, send_sem, recv_sem):
    mine, sibling, across, diagonal = mp_places()
    batch = lax.axis_index("batch")
    to_across, to_sibling = (batch, across), (batch, sibling)
    bias_ref[...] = jnp.broadcast_to(b_in_ref[...].astype(F32), bias_ref.shape)
    greet([to_across, to_sibling])
    pairs = ((w_in_ref, all_in_ref), (w_out_ref, all_out_ref), (bias_ref, all_b_ref))
    far, near, relayed = [], [], []
    for i, (own, whole) in enumerate(pairs):
        copy = send(own, whole.at[mine], send_sem.at[0, i], recv_sem.at[0, i], to_across)
        copy.start()
        far.append(copy)
    for i, (own, whole) in enumerate(pairs):
        copy = send(own, whole.at[mine], send_sem.at[1, i], recv_sem.at[1, i], to_sibling)
        copy.start()
        near.append(copy)
    for own, whole in pairs:
        whole[mine] = own[...]
    for i, (own, whole) in enumerate(pairs):
        far[i].wait_recv()
        copy = send(
            whole.at[across], whole.at[across], send_sem.at[2, i], recv_sem.at[2, i], to_sibling
        )
        copy.start()
        relayed.append(copy)
    for copy in far:
        copy.wait_send()
    for copy in near + relayed:
        copy.wait()


def gather(w_in, w_out, b_in):
    count = lax.axis_size("mp")
    vmem = pl.BlockSpec(memory_space=pltpu.VMEM)
    return pl.pallas_call(
        gather_kernel,
        out_shape=[
            jax.ShapeDtypeStruct((count,) + w_in.shape, BF16),
            jax.ShapeDtypeStruct((count,) + w_out.shape, BF16),
            jax.ShapeDtypeStruct((count, 8, b_in.shape[1]), F32),
        ],
        in_specs=[vmem] * 3,
        out_specs=[vmem] * 3,
        scratch_shapes=[
            pltpu.VMEM((8, b_in.shape[1]), F32),
            pltpu.SemaphoreType.DMA((3, 3)),
            pltpu.SemaphoreType.DMA((3, 3)),
        ],
        compiler_params=pltpu.CompilerParams(
            collective_id=0, has_side_effects=True, vmem_limit_bytes=8 * 1024 * 1024
        ),
        cost_estimate=pl.CostEstimate(flops=0, bytes_accessed=32 << 20, transcendentals=0),
        name="gather_weights",
    )(w_in, w_out, b_in)


def reduce_kernel(
    members,
    total,
    grads_ref,
    done_ref,
    decs_ref,
    near_ref,
    far_w_ref,
    far_t_ref,
    got_w_ref,
    got_t_ref,
    full_ref,
    round_ref,
    parts_ref,
    near_send,
    near_recv,
    far_send,
    far_recv,
    rs_send,
    rs_recv,
    ag_send,
    ag_recv,
    pair_send,
    pair_recv,
    dec_send,
    dec_recv,
):
    mine, sibling, across, diagonal = mp_places()
    batch = lax.axis_index("batch")
    width = grads_ref.shape[2]
    weight_rows = 2 * width
    piece = grads_ref.shape[1] // members
    others = [(lax.rem(batch + d, members), mine) for d in range(1, members)]
    group = [(batch, sibling), (batch, across), (batch, diagonal)]
    greet(group + others)
    near = []
    for i, quarter in enumerate((diagonal, sibling)):
        copy = send(
            grads_ref.at[quarter], near_ref.at[i], near_send.at[i], near_recv.at[i], group[0]
        )
        copy.start()
        near.append(copy)
    near[0].wait_recv()
    far_w_ref[...] = (
        grads_ref[across, :weight_rows, :] + near_ref[0, :weight_rows, :]
    ).astype(BF16)
    far_t_ref[...] = grads_ref[across, weight_rows:, :] + near_ref[0, weight_rows:, :]
    far = [
        send(far_w_ref, got_w_ref, far_send.at[0], far_recv.at[0], group[1]),
        send(far_t_ref, got_t_ref, far_send.at[1], far_recv.at[1], group[1]),
    ]
    for copy in far:
        copy.start()
    near[1].wait_recv()
    full_ref[...] = grads_ref[mine] + near_ref[1]
    far[0].wait_recv()
    full_ref[:weight_rows, :] += got_w_ref[...].astype(F32)
    far[1].wait_recv()
    full_ref[weight_rows:, :] += got_t_ref[...]
    for p in range(members):
        round_ref[p] = full_ref[p * piece : (p + 1) * piece, :].astype(BF16)
    scatter = []
    for d in range(1, members):
        target = lax.rem(batch + d, members)
        copy = send(
            round_ref.at[target],
            parts_ref.at[d - 1],
            rs_send.at[d - 1],
            rs_recv.at[d - 1],
            others[d - 1],
        )
        copy.start()
        scatter.append(copy)
    here = pl.ds(pl.multiple_of(batch * piece, 8), piece)
    value = full_ref[here, :]
    for d in range(1, members):
        scatter[d - 1].wait_recv()
        value = value + parts_ref[d - 1].astype(F32)
    done_ref[here, :] = value / total
    pair = batch + 1 - 2 * (batch % 2)
    partner = (pair, mine)

    def rows_of(owner):
        return done_ref.at[pl.ds(pl.multiple_of(owner * piece, 8), piece), :]

    def relay(i, owner):
        return send(rows_of(owner), rows_of(owner), pair_send.at[i], pair_recv.at[i], partner)

    hops = members // 2
    spread = []
    for d in range(1, hops):
        target = lax.rem(batch + 2 * d, members)
        copy = send(
            rows_of(batch), rows_of(batch), ag_send.at[d - 1], ag_recv.at[d - 1], (target, mine)
        )
        copy.start()
        spread.append(copy)
    passed = [relay(0, batch)]
    passed[0].start()
    for copy in near + far + scatter:
        copy.wait_send()
    for d in range(1, hops):
        origin = lax.rem(batch + members - 2 * d, members)
        send(
            rows_of(origin),
            rows_of(origin),
            ag_send.at[d - 1],
            ag_recv.at[d - 1],
            (origin, mine),
        ).wait_recv()
        copy = relay(d, origin)
        copy.start()
        passed.append(copy)
    for d in range(hops):
        relay(d, lax.rem(pair + members - 2 * d, members)).wait_recv()
    spread += passed
    dec_rows = decs_ref.shape[1]
    exchange = []
    for i in range(3):
        copy = send(
            done_ref.at[pl.ds(weight_rows, dec_rows), :],
            decs_ref.at[mine],
            dec_send.at[i],
            dec_recv.at[i],
            group[i],
        )
        copy.start()
        exchange.append(copy)
    decs_ref[mine] = done_ref[weight_rows : weight_rows + dec_rows, :]
    for copy in spread:
        copy.wait_send()
    for i, origin in enumerate((sibling, across, diagonal)):
        exchange[i].wait_send()
        send(
            decs_ref.at[origin], decs_ref.at[origin], dec_send.at[i], dec_recv.at[i], group[i]
        ).wait_recv()


def finish_kernel(
    half, done_ref, decs_ref, w_in_ref, w_out_ref, b_in_ref, b_out_ref, dec_ref, scores_ref
):
    width = done_ref.shape[1]
    weight_rows = 2 * width
    dec_rows = decs_ref.shape[1]
    line = weight_rows + dec_rows
    w_in_ref[...] = done_ref[:width, :]
    w_out_ref[...] = done_ref[width:weight_rows, :]
    b_in_ref[...] = done_ref[line : line + 1, :]
    b_out_ref[...] = done_ref[line + 1 : line + 2, :]
    scores_ref[:, 0:1] = jnp.sum(done_ref[line + 2 : line + 3, :half], axis=1, keepdims=True)
    scores_ref[:, 1:2] = jnp.sum(
        done_ref[line + 2 : line + 3, half : 2 * half], axis=1, keepdims=True
    )
    seen_width = dec_ref.shape[1]
    for n in range(decs_ref.shape[0]):
        for m in range(width // seen_width):
            start = (n * (width // seen_width) + m) * dec_rows
            dec_ref[start : start + dec_rows, :] = decs_ref[
                n, :, m * seen_width : (m + 1) * seen_width
            ]


def reduce_all(grads, rows, seen_width):
    quarters, grad_rows, width = grads.shape
    members = lax.axis_size("batch")
    total = rows * members * lax.axis_size("mp")
    dec_rows = width // quarters // (width // seen_width)
    tail_rows = grad_rows - 2 * width
    piece = grad_rows // members
    vmem = pl.BlockSpec(memory_space=pltpu.VMEM)
    sems = []
    for count in (2, 2, members - 1, members // 2, members // 2, 3):
        sems += [pltpu.SemaphoreType.DMA((count,))] * 2

    def body(*refs):
        reduce_kernel(members, total, *refs)

    done, decs = pl.pallas_call(
        body,
        out_shape=[
            jax.ShapeDtypeStruct((grad_rows, width), F32),
            jax.ShapeDtypeStruct((quarters, dec_rows, width), F32),
        ],
        in_specs=[vmem],
        out_specs=[vmem] * 2,
        scratch_shapes=[
            pltpu.VMEM((2, grad_rows, width), F32),
            pltpu.VMEM((2 * width, width), BF16),
            pltpu.VMEM((tail_rows, width), F32),
            pltpu.VMEM((2 * width, width), BF16),
            pltpu.VMEM((tail_rows, width), F32),
            pltpu.VMEM((grad_rows, width), F32),
            pltpu.VMEM((members, piece, width), BF16),
            pltpu.VMEM((members - 1, piece, width), BF16),
        ]
        + sems,
        compiler_params=pltpu.CompilerParams(
            collective_id=1, has_side_effects=True, vmem_limit_bytes=16 * 1024 * 1024
        ),
        name="reduce_grads",
    )(grads)

    def finish(*refs):
        finish_kernel(rows, *refs)

    return pl.pallas_call(
        finish,
        out_shape=[
            jax.ShapeDtypeStruct((width, width), F32),
            jax.ShapeDtypeStruct((width, width), F32),
            jax.ShapeDtypeStruct((1, width), F32),
            jax.ShapeDtypeStruct((1, width), F32),
            jax.ShapeDtypeStruct((width, seen_width), F32),
            jax.ShapeDtypeStruct((1, 2), F32),
        ],
        in_specs=[vmem] * 2,
        out_specs=[vmem] * 6,
        compiler_params=pltpu.CompilerParams(vmem_limit_bytes=8 * 1024 * 1024),
        name="finish",
    )(done, decs)


def on_device(
    init_state,
    brownian,
    step_size,
    lengths,
    obs_steps,
    observed,
    w_in,
    b_in,
    w_out,
    b_out,
    decoder,
    prior_rate,
    diffusion,
):
    rows, width = init_state.shape
    seen_width = decoder.shape[1]
    w_in_all, w_out_all, b_in_all = gather(w_in, w_out, b_in[None, :])
    unit = 8 * lax.axis_size("batch")
    need = 2 * width + width // lax.axis_size("mp") * seen_width // width + 3
    elbo, grads, cot = core(
        -(-need // unit) * unit,
        init_state,
        brownian,
        step_size[None, :],
        lengths[None, :],
        obs_steps.T,
        observed,
        w_in_all,
        b_in_all,
        w_out_all,
        b_out[None, :],
        decoder,
        prior_rate[None, :],
        diffusion[None, :],
    )
    own_w_in, own_w_out, own_b_in, b_out_grad, dec_grad, scores = reduce_all(
        grads, rows, seen_width
    )
    return (
        elbo[0],
        scores[0],
        own_w_in,
        own_b_in[0],
        own_w_out,
        b_out_grad[0],
        dec_grad,
        cot,
    )


def solution(mesh):
    both = ("batch", "mp")
    placed = (
        P(both, None),
        P(None, both, None),
        P(both),
        P(both),
        P(both, None),
        P(both, None, None),
        P(None, "mp"),
        P("mp"),
        P("mp", None),
        P(),
        P(),
        P(),
        P(),
    )
    return jax.shard_map(
        on_device,
        mesh=mesh,
        in_specs=placed,
        out_specs=(
            P(both),
            P(),
            P(None, "mp"),
            P("mp"),
            P("mp", None),
            P(),
            P(),
            P(both, None),
        ),
        check_vma=False,
    )
```

```python
import jax
import jax.numpy as jnp
from jax import lax
from jax.experimental import pallas as pl
from jax.experimental.pallas import tpu as pltpu
from jax.sharding import PartitionSpec as P

F32 = jnp.float32
BF16 = jnp.bfloat16
UNITS = (0, 1)
UNROLL = 2


def fold(value):
    return value.reshape(-1, 8, value.shape[1]).sum(axis=0)


def send(source, target, sems, index, peer):
    return pltpu.make_async_remote_copy(
        src_ref=source,
        dst_ref=target,
        send_sem=sems[0].at[index],
        recv_sem=sems[1].at[index],
        device_id=peer,
        device_id_type=pl.DeviceIdType.MESH,
    )


def push(value, slot, unit):
    pltpu.matmul_push_rhs(value, slot, unit)


def multiply(acc, value, slot):
    pltpu.matmul_acc_lhs(acc, value, load_staged_rhs=slot)


class Refs:
    def __init__(self, names, refs):
        for name, ref in zip(names, refs, strict=True):
            setattr(self, name, ref)


def train_kernel(r, members, total_rows):
    rows, width = r.init.shape
    steps = r.noise.shape[0]
    seen_count = r.obs.shape[0]
    seen_width = r.dec.shape[1]
    chunks = r.w_in.shape[0]
    first, second, third, aside, wide = r.first, r.second, r.third, r.aside, r.wide

    mine = lax.axis_index("mp")
    batch = lax.axis_index("batch")
    chip, unit = mine // 2, mine % 2
    sibling = chip * 2 + (1 - unit)
    across = (1 - chip) * 2 + unit
    diagonal = (1 - chip) * 2 + (1 - unit)
    to_sibling, to_across, to_diagonal = (batch, sibling), (batch, across), (batch, diagonal)
    group = (to_sibling, to_across, to_diagonal)
    group_at = (sibling, across, diagonal)
    others_at = [lax.rem(batch + d, members) for d in range(1, members)]
    others = [(at, mine) for at in others_at]
    origins = [lax.rem(batch + members - d, members) for d in range(1, members)]

    loads = {}
    for i, (name, source, target) in enumerate(
        (
            ("w_in", r.w_in_own, r.w_in.at[mine]),
            ("b_in", r.b_in_own, r.b_in_flat),
            ("w_out", r.w_out_own, r.w_out.at[mine]),
            ("step", r.step_hbm, r.step),
            ("length", r.length_hbm, r.length),
            ("obs", r.obs_hbm, r.obs),
            ("init", r.init_hbm, r.init),
            ("b_out", r.b_out_hbm, r.b_out),
            ("dec", r.dec_hbm, r.dec),
            ("rate", r.rate_hbm, r.rate),
            ("diff", r.diff_hbm, r.diff),
            ("noise", r.noise_hbm, r.noise),
            ("seen", r.seen_hbm, r.seen),
        )
    ):
        loads[name] = pltpu.make_async_copy(source, target, r.load_sem.at[i])
        loads[name].start()

    barrier = pltpu.get_barrier_semaphore()
    for peer in list(group) + others:
        pl.semaphore_signal(barrier, inc=1, device_id=peer, device_id_type=pl.DeviceIdType.MESH)
    loads["b_in"].wait()
    r.bias_own[...] = jnp.broadcast_to(
        r.b_in_flat[...].astype(F32).reshape(1, width), r.bias_own.shape
    )
    pl.semaphore_wait(barrier, len(group) + len(others))

    whole = (r.w_in, r.bias, r.w_out)
    own = (r.w_in.at[mine], r.bias_own, r.w_out.at[mine])
    loads["w_in"].wait()
    far, near = [None] * 3, [None] * 3
    for i in (0, 1, 2):
        if i == 2:
            loads["w_out"].wait()
        far[i] = send(own[i], whole[i].at[mine], r.far_sem, i, to_across)
        far[i].start()
        near[i] = send(own[i], whole[i].at[mine], r.near_sem, i, to_sibling)
        near[i].start()
    r.bias[mine] = r.bias_own[...]

    def column(row):
        return jnp.broadcast_to(row, (rows, rows)).T

    for name in ("step", "length", "obs", "init", "b_out", "dec", "rate", "diff"):
        loads[name].wait()
    r.dt[...] = column(r.step[...])
    r.root[...] = jnp.sqrt(r.dt[...])
    r.len_wide[...] = column(r.length[...])
    for j in range(seen_count):
        wide_obs = column(r.obs[j : j + 1, :])
        r.obs_wide[j] = wide_obs
        r.obs_half[j] = wide_obs.astype(F32).astype(BF16)
    r.picked[...] = jnp.zeros_like(r.picked)
    r.kl[...] = jnp.zeros_like(r.kl)
    r.sum_b_in[...] = jnp.zeros_like(r.sum_b_in)
    r.sum_b_out[...] = jnp.zeros_like(r.sum_b_out)
    r.state[...] = r.init[...]
    r.x[0] = r.init[...].astype(BF16)
    r.dec_wide[:, :seen_width] = r.dec[...]
    r.dec_wide[:, seen_width:] = jnp.zeros((width, width - seen_width), BF16)
    dec_t = r.dec[...].T
    r.dec_t[:seen_width, :] = dec_t
    r.dec_t[seen_width:, :] = dec_t
    for u in UNITS:
        for acc in (first[u], second[u], third[u], wide[u]):
            pltpu.matmul_pop(acc)
    pltpu.matmul_pop(aside)

    relayed = []
    for i in (0, 1, 2):
        far[i].wait_recv()
        at = whole[i].at[across]
        copy = send(at, at, r.relay_sem, i, to_sibling)
        copy.start()
        relayed.append(copy)
    loads["noise"].wait()
    loads["seen"].wait()
    r.target[...] = r.seen[...].astype(F32).reshape(r.target.shape)
    for copy in far:
        copy.wait_send()
    for copy in near + relayed:
        copy.wait()

    pair = len(UNITS)
    halves = chunks // pair

    def tile(n):
        return slice(n * width, (n + 1) * width)

    def both(value):
        return jnp.concatenate([value] * (width // rows), axis=1)

    for n in range(chunks):
        r.bias_row[:, tile(n)] = r.bias[n, :1, :]

    def stage_pair(read):
        for slot in range(halves):
            for u in UNITS:
                push(read(slot * pair + u), slot, u)

    def discharge():
        for u in UNITS:
            for slot, acc in ((0, first[u]), (1, second[u])):
                multiply(acc, r.x[0], slot)
                pltpu.matmul_pop(acc)

    def two_phases(x, side, between, later, upcoming):
        for u in UNITS:
            multiply(first[u], x, 0)
        if side is not None:
            push(side[1], 0, 0)
            push(later(1), 0, 1)
        else:
            for u in UNITS:
                push(later(u), 0, u)
        for u in UNITS:
            multiply(second[u], x, 1)
        for u in UNITS:
            push(later(pair + u), 1, u)
        if side is not None:
            multiply(aside, side[0], 0)
            push(later(0), 0, 0)
        for u in UNITS:
            multiply(third[u], between(u, pltpu.matmul_pop(first[u])), 0)
        for u in UNITS:
            push(upcoming(u), 0, u)
        for u in UNITS:
            multiply(third[u], between(pair + u, pltpu.matmul_pop(second[u])), 1)
        for u in UNITS:
            push(upcoming(pair + u), 1, u)
        extra = pltpu.matmul_pop(aside) if side is not None else None
        return pltpu.matmul_pop(third[0]) + pltpu.matmul_pop(third[1]), extra

    def pick(index, x):
        at = jnp.full((1, 1), index, jnp.int32).astype(F32).astype(BF16)
        for j in range(seen_count):
            hit = r.obs_half[j] == at
            for m in range(width // rows):
                lanes = slice(m * rows, (m + 1) * rows)
                r.picked[j, :, lanes] = jnp.where(hit, x[:, lanes], r.picked[j, :, lanes])

    def forward(k, carry):
        x = r.x[k]

        def between(n, raw):
            act = jnp.tanh(raw + r.bias_row[:, tile(n)]).astype(BF16)
            r.act[pl.ds(k * rows, rows), tile(n)] = act
            return act

        total, _ = two_phases(x, None, between, lambda n: r.w_out[n], lambda n: r.w_in[n])
        drift = total + r.b_out[...]
        state = r.state[...]
        inv = 1.0 / r.diff[...]
        live = k < r.len_wide[...]
        factor = both(jnp.where(live, r.dt[...], 0.0))
        root = both(jnp.where(live, r.root[...], 0.0))
        following = state + (factor * drift + r.diff[...] * root * r.noise[k].astype(F32))
        r.state[...] = following
        r.x[k + 1] = following.astype(BF16)
        residual = (drift + r.rate[...] * state) * inv
        r.kl[...] += factor * residual * residual
        r.scaled[k] = residual * inv
        r.xt[:, pl.ds(pl.multiple_of(k * rows, rows), rows)] = x.T
        pick(k, x)
        return carry

    stage_pair(lambda n: r.w_in[n])
    lax.fori_loop(0, steps, forward, 0, unroll=UNROLL)
    discharge()
    pick(steps, r.x[steps])

    square = jnp.zeros((rows, seen_width), F32)
    seen_accs = (first[0], first[1], second[0], second[1])
    for u in UNITS:
        push(r.dec_wide[...], 0, u)
    loaded = [False, False]
    for start in range(0, seen_count, len(seen_accs)):
        batch_j = list(range(start, min(start + len(seen_accs), seen_count)))
        for at, (acc, j) in enumerate(zip(seen_accs, batch_j)):
            u = at % 2
            multiply(acc, r.picked[j], None if loaded[u] else 0)
            loaded[u] = True
        for acc, j in zip(seen_accs, batch_j):
            misfit = (
                pltpu.matmul_pop(acc)[:, :seen_width]
                - r.target[pl.ds(j, rows, stride=seen_count), :]
            )
            square = square + misfit * misfit
            rounded = misfit.astype(BF16)
            r.misfit[j] = rounded.astype(F32)
            r.misfit_wide[j * rows : (j + 1) * rows, :seen_width] = rounded
    r.misfit_wide[:, seen_width:] = jnp.zeros(
        (seen_count * rows, width - seen_width), BF16
    )
    per = width // rows
    for p in range(seen_count // per):
        u = p % 2
        left = jnp.concatenate([r.picked[p * per + m].T for m in range(per)], axis=1)
        push(r.misfit_wide[p * width : (p + 1) * width, :], 0, u)
        multiply(wide[u], left, 0)
    dec_grad = (pltpu.matmul_pop(wide[0]) + pltpu.matmul_pop(wide[1]))[:, :seen_width]
    loglik = -0.5 * jnp.sum(square.T, axis=0, keepdims=True)
    kl_half = r.kl[:, :rows]
    for part in range(1, width // rows):
        kl_half = kl_half + r.kl[:, part * rows : (part + 1) * rows]
    kl_row = 0.5 * jnp.sum(kl_half.T, axis=0, keepdims=True)
    divisor = (width * r.length[...] + seen_width * seen_count).astype(F32)
    r.elbo[...] = (loglik - kl_row) / divisor

    quarter = width // chunks
    score_rows = jnp.concatenate(
        [loglik, kl_row, jnp.zeros((6, rows), F32)], axis=0
    )
    for n in range(chunks):
        r.dec_part[n, :quarter, :] = dec_grad[n * quarter : (n + 1) * quarter, :]
        r.dec_part[n, quarter:, :] = score_rows
    dec_first = []
    for i, (peer, at) in enumerate(zip(group, group_at)):
        copy = send(r.dec_part.at[at], r.dec_got.at[i], r.dec_sem, i, peer)
        copy.start()
        dec_first.append(copy)

    for n in range(chunks):
        r.w_in_t[n] = r.w_in[n].T
        r.w_out_t[n] = r.w_out[n].T

    def obs_sum(index):
        total = jnp.zeros((rows, seen_width), F32)
        for j in range(seen_count):
            total = total + jnp.where(r.obs_wide[j] == index, r.misfit[j], 0.0)
        high = total.astype(BF16)
        low = (total - high.astype(F32)).astype(BF16)
        return jnp.concatenate([high, low], axis=1)

    push(r.dec_t[...], 0, 0)
    multiply(aside, obs_sum(steps), 0)
    r.cot[...] = pltpu.matmul_pop(aside)
    stage_pair(lambda n: r.w_out_t[n])

    def backward(index, carry):
        k = steps - 1 - index
        cot = r.cot[...]
        scaled = r.scaled[k]
        factor = both(jnp.where(k < r.len_wide[...], r.dt[...], 0.0))
        update = factor * (cot + scaled)
        rounded = update.astype(BF16)

        def between(n, raw):
            act = r.act[pl.ds(k * rows, rows), tile(n)].astype(F32)
            pre = raw * (1.0 - act * act)
            pre_round = pre.astype(BF16)
            r.pre[pl.ds(k * rows, rows), tile(n)] = pre_round
            r.sum_b_in[:, tile(n)] += fold(pre)
            return pre_round

        total, seen_back = two_phases(
            rounded,
            (obs_sum(k), r.dec_t[...]),
            between,
            lambda n: r.w_in_t[n],
            lambda n: r.w_out_t[n],
        )
        r.cot[...] = total + (cot + factor * r.rate[...] * scaled + seen_back)
        r.ut[:, pl.ds(pl.multiple_of(k * rows, rows), rows)] = rounded.T
        r.sum_b_out[...] += fold(update)
        return carry

    cut_a, cut_b = steps * 3 // 8 // 2 * 2, steps * 6 // 8 // 2 * 2
    lax.fori_loop(0, cut_a, backward, 0, unroll=UNROLL)
    for copy in dec_first:
        copy.wait_recv()
    dec_sum = r.dec_part[mine]
    for i in range(len(group)):
        dec_sum = dec_sum + r.dec_got[i]
    r.dec_mid[batch] = dec_sum
    dec_second = []
    for d, peer in enumerate(others):
        copy = send(r.dec_mid.at[batch], r.dec_mid.at[batch], r.dec_all_sem, d, peer)
        copy.start()
        dec_second.append(copy)
    lax.fori_loop(cut_a, cut_b, backward, 0, unroll=UNROLL)
    for d, origin in enumerate(origins):
        send(
            r.dec_mid.at[origin], r.dec_mid.at[origin], r.dec_all_sem, d, (origin, mine)
        ).wait_recv()
    dec_total = r.dec_mid[0]
    for b in range(1, members):
        dec_total = dec_total + r.dec_mid[b]
    r.decs[mine] = dec_total / total_rows
    dec_third = []
    for i, peer in enumerate(group):
        copy = send(r.decs.at[mine], r.decs.at[mine], r.dec_out_sem, i, peer)
        copy.start()
        dec_third.append(copy)
    lax.fori_loop(cut_b, steps, backward, 0, unroll=UNROLL)
    discharge()

    b_out_sum = jnp.sum(r.sum_b_out[...], axis=0, keepdims=True)
    pad = jnp.zeros((6, width), F32)
    for n in range(chunks):
        b_in_sum = jnp.sum(r.sum_b_in[:, tile(n)], axis=0, keepdims=True)
        r.b_part[n] = jnp.concatenate([b_in_sum, b_out_sum, pad], axis=0)
    r.b_got[mine] = r.b_part[mine]
    b_first = []
    for i, (peer, at) in enumerate(zip(group, group_at)):
        copy = send(r.b_part.at[at], r.b_got.at[mine], r.b_sem, i, peer)
        copy.start()
        b_first.append(copy)

    depth = width
    parts = steps * rows // depth
    sources = ((r.xt, r.pre), (r.ut, r.act))

    def products(t, quarters):
        left_ref, right_ref = sources[t]
        for p in range(parts):
            k_rows = slice(p * depth, (p + 1) * depth)
            for u, n in zip(UNITS, quarters):
                lanes = pl.ds(pl.multiple_of(n * width, width), width)
                push(right_ref[k_rows, lanes], p % 2, u)
                multiply(wide[u], left_ref[:, k_rows], p % 2)
        return [pltpu.matmul_pop(wide[u]) for u in UNITS]

    near_copies = []

    def exchange(t):
        for i, quarters in enumerate(((diagonal, across), (sibling, mine))):
            away, keep = products(t, quarters)
            r.near_out[t, i] = away
            copy = send(
                r.near_out.at[t, i], r.near_in.at[t, i], r.grad_sem, 2 * t + i, to_sibling
            )
            copy.start()
            near_copies.append(copy)
            r.keep[t, i] = keep

    far_copies = []

    def cross(t):
        near_copies[2 * t].wait_recv()
        r.far_out[t] = (r.keep[t, 0] + r.near_in[t, 0]).astype(BF16)
        copy = send(r.far_out.at[t], r.far_in.at[t], r.cross_sem, t, to_across)
        copy.start()
        far_copies.append(copy)

    piece = width // members
    scatter_copies = [[], []]

    def scatter(t):
        near_copies[2 * t + 1].wait_recv()
        far_copies[t].wait_recv()
        full = r.keep[t, 1] + r.near_in[t, 1] + r.far_in[t].astype(F32)
        r.full[t] = full.reshape(members, piece, width)
        r.scatter_out[t] = full.astype(BF16).reshape(members, piece, width)
        for d, (peer, at) in enumerate(zip(others, others_at)):
            copy = send(
                r.scatter_out.at[t, at],
                r.scatter_in.at[t, d],
                r.scatter_sem,
                t * (members - 1) + d,
                peer,
            )
            copy.start()
            scatter_copies[t].append(copy)

    spread_copies = []

    def spread(t):
        value = r.full[t, batch]
        for d in range(members - 1):
            scatter_copies[t][d].wait_recv()
            value = value + r.scatter_in[t, d].astype(F32)
        r.done[t, batch] = (value / total_rows).astype(BF16)
        for d, peer in enumerate(others):
            copy = send(
                r.done.at[t, batch],
                r.done.at[t, batch],
                r.spread_sem,
                t * (members - 1) + d,
                peer,
            )
            copy.start()
            spread_copies.append(copy)

    def collect(t):
        for d, origin in enumerate(origins):
            send(
                r.done.at[t, origin],
                r.done.at[t, origin],
                r.spread_sem,
                t * (members - 1) + d,
                (origin, mine),
            ).wait_recv()

    exchange(0)
    cross(0)
    exchange(1)
    cross(1)
    for i, (peer, at) in enumerate(zip(group, group_at)):
        send(r.b_part.at[at], r.b_got.at[at], r.b_sem, i, peer).wait_recv()
    b_sum = r.b_got[0]
    for n in range(1, chunks):
        b_sum = b_sum + r.b_got[n]
    r.b_mid[batch] = b_sum
    b_second = []
    for d, peer in enumerate(others):
        copy = send(r.b_mid.at[batch], r.b_mid.at[batch], r.b_all_sem, d, peer)
        copy.start()
        b_second.append(copy)
    scatter(0)
    scatter(1)
    spread(0)
    spread(1)
    for i, (peer, at) in enumerate(zip(group, group_at)):
        send(r.decs.at[at], r.decs.at[at], r.dec_out_sem, i, peer).wait_recv()
    for d, origin in enumerate(origins):
        send(
            r.b_mid.at[origin], r.b_mid.at[origin], r.b_all_sem, d, (origin, mine)
        ).wait_recv()
    b_total = r.b_mid[0]
    for b in range(1, members):
        b_total = b_total + r.b_mid[b]
    r.b_done[...] = b_total / total_rows
    for copy in (
        dec_first + dec_second + dec_third + b_first + b_second + near_copies + far_copies
    ):
        copy.wait_send()
    for copy in scatter_copies[0] + scatter_copies[1]:
        copy.wait_send()
    collect(0)
    collect(1)
    for copy in spread_copies:
        copy.wait_send()


def finish_kernel(
    done_ref,
    b_ref,
    decs_ref,
    cot_ref,
    elbo_ref,
    w_in_out,
    w_out_out,
    b_in_out,
    b_out_out,
    dec_out,
    scores_out,
    cot_out,
    elbo_out,
):
    _, members, piece, width = done_ref.shape
    for b in range(members):
        part = slice(b * piece, (b + 1) * piece)
        w_in_out[part, :] = done_ref[0, b].astype(F32)
    w_out_out[...] = done_ref[1].astype(F32).reshape(members * piece, width).T
    b_in_out[...] = b_ref[0:1, :]
    b_out_out[...] = b_ref[1:2, :]
    quarter = dec_out.shape[0] // decs_ref.shape[0]
    for n in range(decs_ref.shape[0]):
        dec_out[n * quarter : (n + 1) * quarter, :] = decs_ref[n, :quarter, :]
    likelihood = jnp.zeros((1, 1), F32)
    divergence = jnp.zeros((1, 1), F32)
    for n in range(decs_ref.shape[0]):
        share = decs_ref[n, quarter : quarter + 2, :]
        likelihood = share[0:1] if n == 0 else likelihood
        divergence = share[1:2] if n == 0 else divergence
    scores_out[:, 0:1] = jnp.sum(likelihood, axis=1, keepdims=True)
    scores_out[:, 1:2] = jnp.sum(divergence, axis=1, keepdims=True)
    cot_out[...] = cot_ref[...]
    elbo_out[...] = elbo_ref[...]


def on_device(
    init_state,
    brownian,
    step_size,
    lengths,
    obs_steps,
    observed,
    w_in,
    b_in,
    w_out,
    b_out,
    decoder,
    prior_rate,
    diffusion,
):
    rows, width = init_state.shape
    steps = brownian.shape[0]
    seen_count, seen_width = observed.shape[1:]
    chunks, members = lax.axis_size("mp"), lax.axis_size("batch")
    quarter = width // chunks
    piece = width // members
    total_rows = rows * chunks * members
    hidden = chunks * width
    hbm = pl.BlockSpec(memory_space=pltpu.HBM)
    vmem = pl.BlockSpec(memory_space=pltpu.VMEM)

    inputs = {
        "init_hbm": init_state,
        "noise_hbm": brownian,
        "step_hbm": step_size[None, :],
        "length_hbm": lengths[None, :],
        "obs_hbm": obs_steps.T,
        "seen_hbm": observed,
        "w_in_own": w_in,
        "b_in_own": b_in,
        "w_out_own": w_out,
        "b_out_hbm": b_out[None, :],
        "dec_hbm": decoder,
        "rate_hbm": prior_rate[None, :],
        "diff_hbm": diffusion[None, :],
    }
    outputs = {
        "done": ((2, members, piece, width), BF16),
        "b_done": ((8, width), F32),
        "decs": ((chunks, quarter + 8, seen_width), F32),
        "cot": ((rows, width), F32),
        "elbo": ((1, rows), F32),
    }
    scratch = {
        "init": ((rows, width), F32),
        "noise": ((steps, rows, width), BF16),
        "step": ((1, rows), F32),
        "length": ((1, rows), jnp.int32),
        "obs": ((seen_count, rows), jnp.int32),
        "seen": ((rows, seen_count, seen_width), BF16),
        "w_in": ((chunks, width, width), BF16),
        "w_out": ((chunks, width, width), BF16),
        "b_in_flat": ((width,), BF16),
        "bias_own": ((8, width), F32),
        "bias": ((chunks, 8, width), F32),
        "bias_row": ((1, hidden), F32),
        "b_out": ((1, width), F32),
        "dec": ((width, seen_width), BF16),
        "rate": ((1, width), F32),
        "diff": ((1, width), F32),
        "w_in_t": ((chunks, width, width), BF16),
        "w_out_t": ((chunks, width, width), BF16),
        "dec_wide": ((width, width), BF16),
        "dec_t": ((2 * seen_width, width), BF16),
        "dt": ((rows, rows), F32),
        "root": ((rows, rows), F32),
        "len_wide": ((rows, rows), jnp.int32),
        "obs_wide": ((seen_count, rows, rows), jnp.int32),
        "obs_half": ((seen_count, rows, rows), BF16),
        "picked": ((seen_count, rows, width), BF16),
        "misfit": ((seen_count, rows, seen_width), F32),
        "misfit_wide": ((seen_count * rows, width), BF16),
        "target": ((rows * seen_count, seen_width), F32),
        "state": ((rows, width), F32),
        "kl": ((rows, width), F32),
        "sum_b_in": ((8, hidden), F32),
        "sum_b_out": ((8, width), F32),
        "x": ((steps + 1, rows, width), BF16),
        "xt": ((width, steps * rows), BF16),
        "ut": ((width, steps * rows), BF16),
        "act": ((steps * rows, hidden), BF16),
        "pre": ((steps * rows, hidden), BF16),
        "scaled": ((steps, rows, width), F32),
        "dec_part": ((chunks, quarter + 8, seen_width), F32),
        "dec_got": ((3, quarter + 8, seen_width), F32),
        "dec_mid": ((members, quarter + 8, seen_width), F32),
        "b_part": ((chunks, 8, width), F32),
        "b_got": ((chunks, 8, width), F32),
        "b_mid": ((members, 8, width), F32),
        "near_out": ((2, 2, width, width), F32),
        "near_in": ((2, 2, width, width), F32),
        "keep": ((2, 2, width, width), F32),
        "far_out": ((2, width, width), BF16),
        "far_in": ((2, width, width), BF16),
        "full": ((2, members, piece, width), F32),
        "scatter_out": ((2, members, piece, width), BF16),
        "scatter_in": ((2, members - 1, piece, width), BF16),
    }
    waits = {
        "far_sem": 3,
        "near_sem": 3,
        "relay_sem": 3,
        "dec_sem": 3,
        "dec_all_sem": members - 1,
        "dec_out_sem": 3,
        "b_sem": 3,
        "b_all_sem": members - 1,
        "grad_sem": 4,
        "cross_sem": 2,
        "scatter_sem": 2 * (members - 1),
        "spread_sem": 2 * (members - 1),
    }

    def body(*refs):
        refs = list(refs)
        named = Refs(
            list(inputs) + list(outputs) + list(scratch),
            refs[: len(inputs) + len(outputs) + len(scratch)],
        )
        sems = refs[len(inputs) + len(outputs) + len(scratch) :]
        named.load_sem = sems.pop(0)
        for name in waits:
            setattr(named, name, (sems.pop(0), sems.pop(0)))

        def with_accs(*accs):
            named.first, named.second, named.third = accs[0:2], accs[2:4], accs[4:6]
            named.wide, named.aside = accs[6:8], accs[8]
            train_kernel(named, members, total_rows)

        pl.run_scoped(
            with_accs,
            *[pltpu.ACC(u)((rows, width), F32) for _ in range(3) for u in UNITS],
            *[pltpu.ACC(u)((width, width), F32) for u in UNITS],
            pltpu.ACC(0)((rows, width), F32),
        )

    sem_shapes = [pltpu.SemaphoreType.DMA((len(inputs),))]
    for count in waits.values():
        sem_shapes += [pltpu.SemaphoreType.DMA((count,))] * 2
    done, b_done, decs, cot, elbo = pl.pallas_call(
        body,
        out_shape=[jax.ShapeDtypeStruct(*s) for s in outputs.values()],
        in_specs=[hbm] * len(inputs),
        out_specs=[vmem] * len(outputs),
        scratch_shapes=[pltpu.VMEM(*s) for s in scratch.values()] + sem_shapes,
        compiler_params=pltpu.CompilerParams(
            collective_id=0, has_side_effects=True, vmem_limit_bytes=58 * 1024 * 1024
        ),
        name="train",
    )(*inputs.values())
    results = pl.pallas_call(
        finish_kernel,
        out_shape=[
            jax.ShapeDtypeStruct((width, width), F32),
            jax.ShapeDtypeStruct((width, width), F32),
            jax.ShapeDtypeStruct((1, width), F32),
            jax.ShapeDtypeStruct((1, width), F32),
            jax.ShapeDtypeStruct((width, seen_width), F32),
            jax.ShapeDtypeStruct((1, 2), F32),
            jax.ShapeDtypeStruct((rows, width), F32),
            jax.ShapeDtypeStruct((1, rows), F32),
        ],
        in_specs=[vmem] * 5,
        out_specs=[vmem] * 8,
        compiler_params=pltpu.CompilerParams(vmem_limit_bytes=4 * 1024 * 1024),
        name="finish",
    )(done, b_done, decs, cot, elbo)
    own_w_in, own_w_out, own_b_in, b_out_grad, dec_grad, scores, grad_init, elbo = results
    return (
        elbo[0],
        scores[0],
        own_w_in,
        own_b_in[0],
        own_w_out,
        b_out_grad[0],
        dec_grad,
        grad_init,
    )


def solution(mesh):
    both = ("batch", "mp")
    placed = (
        P(both, None),
        P(None, both, None),
        P(both),
        P(both),
        P(both, None),
        P(both, None, None),
        P(None, "mp"),
        P("mp"),
        P("mp", None),
        P(),
        P(),
        P(),
        P(),
    )
    return jax.shard_map(
        on_device,
        mesh=mesh,
        in_specs=placed,
        out_specs=(
            P(both),
            P(),
            P(None, "mp"),
            P("mp"),
            P("mp", None),
            P(),
            P(),
            P(both, None),
        ),
        check_vma=False,
    )
```

```python
import jax
import jax.numpy as jnp
from jax import lax
from jax.experimental import pallas as pl
from jax.experimental.pallas import tpu as pltpu
from jax.sharding import PartitionSpec as P

F32 = jnp.float32
BF16 = jnp.bfloat16
UNITS = (0, 1)
UNROLL = 2
LIMIT = 48 * 1024 * 1024


def fold(value):
    return value.reshape(-1, 8, value.shape[1]).sum(axis=0)


def send(source, target, sems, index, peer):
    return pltpu.make_async_remote_copy(
        src_ref=source,
        dst_ref=target,
        send_sem=sems[0].at[index],
        recv_sem=sems[1].at[index],
        device_id=peer,
        device_id_type=pl.DeviceIdType.MESH,
    )


def push(value, slot, unit):
    pltpu.matmul_push_rhs(value, slot, unit)


def multiply(acc, value, slot):
    pltpu.matmul_acc_lhs(acc, value, load_staged_rhs=slot)


class Refs:
    def __init__(self, names, refs):
        for name, ref in zip(names, refs, strict=True):
            setattr(self, name, ref)


def train_kernel(r, members, total_rows):
    rows, width = r.init.shape
    steps = r.noise.shape[0]
    seen_count = r.obs.shape[0]
    seen_width = r.dec.shape[1]
    chunks = r.w_in.shape[0]
    first, second, third, aside, wide = r.first, r.second, r.third, r.aside, r.wide

    mine = lax.axis_index("mp")
    batch = lax.axis_index("batch")
    chip, unit = mine // 2, mine % 2
    sibling = chip * 2 + (1 - unit)
    across = (1 - chip) * 2 + unit
    diagonal = (1 - chip) * 2 + (1 - unit)
    to_sibling, to_across, to_diagonal = (batch, sibling), (batch, across), (batch, diagonal)
    group = (to_sibling, to_across, to_diagonal)
    group_at = (sibling, across, diagonal)
    others_at = [lax.rem(batch + d, members) for d in range(1, members)]
    others = [(at, mine) for at in others_at]
    origins = [lax.rem(batch + members - d, members) for d in range(1, members)]

    loads = {}
    for i, (name, source, target) in enumerate(
        (
            ("w_in", r.w_in_own, r.w_in.at[mine]),
            ("b_in", r.b_in_own, r.b_in_flat),
            ("w_out", r.w_out_own, r.w_out.at[mine]),
            ("step", r.step_hbm, r.step),
            ("length", r.length_hbm, r.length),
            ("obs", r.obs_hbm, r.obs),
            ("init", r.init_hbm, r.init),
            ("b_out", r.b_out_hbm, r.b_out),
            ("dec", r.dec_hbm, r.dec),
            ("rate", r.rate_hbm, r.rate),
            ("diff", r.diff_hbm, r.diff),
            ("noise", r.noise_hbm, r.noise),
            ("seen", r.seen_hbm, r.seen),
        )
    ):
        loads[name] = pltpu.make_async_copy(source, target, r.load_sem.at[i])
        loads[name].start()

    barrier = pltpu.get_barrier_semaphore()
    for peer in list(group) + others:
        pl.semaphore_signal(barrier, inc=1, device_id=peer, device_id_type=pl.DeviceIdType.MESH)
    loads["b_in"].wait()
    r.bias_own[...] = jnp.broadcast_to(
        r.b_in_flat[...].astype(F32).reshape(1, width), r.bias_own.shape
    )
    pl.semaphore_wait(barrier, len(group) + len(others))

    whole = (r.w_in, r.bias, r.w_out)
    own = (r.w_in.at[mine], r.bias_own, r.w_out.at[mine])
    loads["w_in"].wait()
    far, near = [None] * 3, [None] * 3
    for i in (0, 1, 2):
        if i == 2:
            loads["w_out"].wait()
        far[i] = send(own[i], whole[i].at[mine], r.far_sem, i, to_across)
        far[i].start()
        near[i] = send(own[i], whole[i].at[mine], r.near_sem, i, to_sibling)
        near[i].start()
    r.bias[mine] = r.bias_own[...]

    def column(row):
        return jnp.broadcast_to(row, (rows, rows)).T

    for name in ("step", "length", "obs", "init", "b_out", "dec", "rate", "diff"):
        loads[name].wait()
    r.dt[...] = column(r.step[...])
    r.root[...] = jnp.sqrt(r.dt[...])
    r.len_wide[...] = column(r.length[...])
    for j in range(seen_count):
        wide_obs = column(r.obs[j : j + 1, :])
        r.obs_wide[j] = wide_obs
        r.obs_half[j] = wide_obs.astype(jnp.int16)
    r.kl[...] = jnp.zeros_like(r.kl)
    r.sum_b_in[...] = jnp.zeros_like(r.sum_b_in)
    r.sum_b_out[...] = jnp.zeros_like(r.sum_b_out)
    r.state[...] = r.init[...]
    r.x[0] = r.init[...].astype(BF16)
    r.dec_wide[:, :seen_width] = r.dec[...]
    r.dec_wide[:, seen_width:] = jnp.zeros((width, width - seen_width), BF16)
    dec_t = r.dec[...].T
    r.dec_t[:seen_width, :] = dec_t
    r.dec_t[seen_width:, :] = dec_t
    for u in UNITS:
        for acc in (first[u], second[u], third[u], wide[u]):
            pltpu.matmul_pop(acc)
    pltpu.matmul_pop(aside)

    relayed = []
    for i in (0, 1, 2):
        far[i].wait_recv()
        at = whole[i].at[across]
        copy = send(at, at, r.relay_sem, i, to_sibling)
        copy.start()
        relayed.append(copy)
    loads["noise"].wait()
    loads["seen"].wait()
    r.target[...] = r.seen[...].astype(F32).reshape(r.target.shape)
    for copy in far:
        copy.wait_send()
    for copy in near + relayed:
        copy.wait()

    pair = len(UNITS)
    halves = chunks // pair

    def tile(n):
        return slice(n * width, (n + 1) * width)

    def both(value):
        return jnp.concatenate([value] * (width // rows), axis=1)

    for n in range(chunks):
        r.bias_row[:, tile(n)] = r.bias[n, :1, :]

    def stage_pair(read):
        for slot in range(halves):
            for u in UNITS:
                push(read(slot * pair + u), slot, u)

    def discharge():
        for u in UNITS:
            for slot, acc in ((0, first[u]), (1, second[u])):
                multiply(acc, r.x[0], slot)
                pltpu.matmul_pop(acc)

    def two_phases(x, side, between, later, upcoming):
        for u in UNITS:
            multiply(first[u], x, 0)
        if side is not None:
            push(side[1], 0, 0)
            push(later(1), 0, 1)
        else:
            for u in UNITS:
                push(later(u), 0, u)
        for u in UNITS:
            multiply(second[u], x, 1)
        for u in UNITS:
            push(later(pair + u), 1, u)
        if side is not None:
            multiply(aside, side[0], 0)
            push(later(0), 0, 0)
        for u in UNITS:
            multiply(third[u], between(u, pltpu.matmul_pop(first[u])), 0)
        for u in UNITS:
            push(upcoming(u), 0, u)
        for u in UNITS:
            multiply(third[u], between(pair + u, pltpu.matmul_pop(second[u])), 1)
        for u in UNITS:
            push(upcoming(pair + u), 1, u)
        extra = pltpu.matmul_pop(aside) if side is not None else None
        return pltpu.matmul_pop(third[0]) + pltpu.matmul_pop(third[1]), extra

    band = 16

    def pick_band(b, carry):
        at = pl.ds(pl.multiple_of(b * band, band), band)
        wanted = [r.obs_half[j, at, :] for j in range(seen_count)]

        def look(k, found):
            x = r.x[k, at, :]
            index = jnp.full((band, rows), k, jnp.int32).astype(jnp.int16)
            out = []
            for j in range(seen_count):
                hit = wanted[j] == index
                for m in range(width // rows):
                    at_m = j * (width // rows) + m
                    out.append(jnp.where(hit, x[:, m * rows : (m + 1) * rows], found[at_m]))
            return tuple(out)

        blank = jnp.zeros((band, rows), BF16)
        found = lax.fori_loop(
            1, steps + 1, look, (blank,) * (seen_count * (width // rows)), unroll=4
        )
        for j in range(seen_count):
            for m in range(width // rows):
                r.picked[j, at, m * rows : (m + 1) * rows] = found[j * (width // rows) + m]
        return carry

    def forward(k, carry):
        x = r.x[k]

        def between(n, raw):
            act = jnp.tanh(raw + r.bias_row[:, tile(n)]).astype(BF16)
            r.act[pl.ds(k * rows, rows), tile(n)] = act
            return act

        total, _ = two_phases(x, None, between, lambda n: r.w_out[n], lambda n: r.w_in[n])
        drift = total + r.b_out[...]
        state = r.state[...]
        inv = 1.0 / r.diff[...]
        live = k < r.len_wide[...]
        factor = both(jnp.where(live, r.dt[...], 0.0))
        root = both(jnp.where(live, r.root[...], 0.0))
        following = state + (factor * drift + r.diff[...] * root * r.noise[k].astype(F32))
        r.state[...] = following
        r.x[k + 1] = following.astype(BF16)
        residual = (drift + r.rate[...] * state) * inv
        r.kl[...] += factor * residual * residual
        r.scaled[k] = residual * inv
        r.xt[:, pl.ds(pl.multiple_of(k * rows, rows), rows)] = x.T
        return carry

    stage_pair(lambda n: r.w_in[n])
    lax.fori_loop(0, steps, forward, 0, unroll=UNROLL)
    discharge()
    lax.fori_loop(0, rows // band, pick_band, 0)

    square = jnp.zeros((rows, seen_width), F32)
    seen_accs = (first[0], first[1], second[0], second[1])
    for u in UNITS:
        push(r.dec_wide[...], 0, u)
    loaded = [False, False]
    for start in range(0, seen_count, len(seen_accs)):
        batch_j = list(range(start, min(start + len(seen_accs), seen_count)))
        for at, (acc, j) in enumerate(zip(seen_accs, batch_j)):
            u = at % 2
            multiply(acc, r.picked[j], None if loaded[u] else 0)
            loaded[u] = True
        for acc, j in zip(seen_accs, batch_j):
            misfit = (
                pltpu.matmul_pop(acc)[:, :seen_width]
                - r.target[pl.ds(j, rows, stride=seen_count), :]
            )
            square = square + misfit * misfit
            rounded = misfit.astype(BF16)
            r.misfit[j] = rounded.astype(F32)
            r.misfit_wide[j * rows : (j + 1) * rows, :seen_width] = rounded
    r.misfit_wide[:, seen_width:] = jnp.zeros(
        (seen_count * rows, width - seen_width), BF16
    )
    per = width // rows
    for p in range(seen_count // per):
        u = p % 2
        left = jnp.concatenate([r.picked[p * per + m].T for m in range(per)], axis=1)
        push(r.misfit_wide[p * width : (p + 1) * width, :], 0, u)
        multiply(wide[u], left, 0)
    dec_grad = (pltpu.matmul_pop(wide[0]) + pltpu.matmul_pop(wide[1]))[:, :seen_width]
    loglik = -0.5 * jnp.sum(square.T, axis=0, keepdims=True)
    kl_half = r.kl[:, :rows]
    for part in range(1, width // rows):
        kl_half = kl_half + r.kl[:, part * rows : (part + 1) * rows]
    kl_row = 0.5 * jnp.sum(kl_half.T, axis=0, keepdims=True)
    divisor = (width * r.length[...] + seen_width * seen_count).astype(F32)
    r.elbo[...] = (loglik - kl_row) / divisor

    quarter = width // chunks
    score_rows = jnp.concatenate(
        [loglik, kl_row, jnp.zeros((6, rows), F32)], axis=0
    )
    for n in range(chunks):
        r.dec_part[n, :quarter, :] = dec_grad[n * quarter : (n + 1) * quarter, :]
        r.dec_part[n, quarter:, :] = score_rows
    dec_first = []
    for i, (peer, at) in enumerate(zip(group, group_at)):
        copy = send(r.dec_part.at[at], r.dec_got.at[i], r.dec_sem, i, peer)
        copy.start()
        dec_first.append(copy)

    for n in range(chunks):
        r.w_in_t[n] = r.w_in[n].T
        r.w_out_t[n] = r.w_out[n].T

    def obs_sum(index):
        total = jnp.zeros((rows, seen_width), F32)
        for j in range(seen_count):
            total = total + jnp.where(r.obs_wide[j] == index, r.misfit[j], 0.0)
        high = total.astype(BF16)
        low = (total - high.astype(F32)).astype(BF16)
        return jnp.concatenate([high, low], axis=1)

    push(r.dec_t[...], 0, 0)
    multiply(aside, obs_sum(steps), 0)
    r.cot[...] = pltpu.matmul_pop(aside)
    stage_pair(lambda n: r.w_out_t[n])

    def backward(index, carry):
        k = steps - 1 - index
        cot = r.cot[...]
        scaled = r.scaled[k]
        factor = both(jnp.where(k < r.len_wide[...], r.dt[...], 0.0))
        update = factor * (cot + scaled)
        rounded = update.astype(BF16)

        def between(n, raw):
            act = r.act[pl.ds(k * rows, rows), tile(n)].astype(F32)
            pre = raw * (1.0 - act * act)
            pre_round = pre.astype(BF16)
            r.pre[pl.ds(k * rows, rows), tile(n)] = pre_round
            r.sum_b_in[:, tile(n)] += fold(pre)
            return pre_round

        total, seen_back = two_phases(
            rounded,
            (obs_sum(k), r.dec_t[...]),
            between,
            lambda n: r.w_in_t[n],
            lambda n: r.w_out_t[n],
        )
        r.cot[...] = total + (cot + factor * r.rate[...] * scaled + seen_back)
        r.ut[:, pl.ds(pl.multiple_of(k * rows, rows), rows)] = rounded.T
        r.sum_b_out[...] += fold(update)
        return carry

    cut = steps * 3 // 8 // 2 * 2
    lax.fori_loop(0, cut, backward, 0, unroll=UNROLL)
    for copy in dec_first:
        copy.wait_recv()
    dec_sum = r.dec_part[mine]
    for i in range(len(group)):
        dec_sum = dec_sum + r.dec_got[i]
    r.dec_mid[batch] = dec_sum
    dec_second = []
    for d, peer in enumerate(others):
        copy = send(r.dec_mid.at[batch], r.dec_mid.at[batch], r.dec_all_sem, d, peer)
        copy.start()
        dec_second.append(copy)
    lax.fori_loop(cut, steps, backward, 0, unroll=UNROLL)
    discharge()

    b_out_sum = jnp.sum(r.sum_b_out[...], axis=0, keepdims=True)
    pad = jnp.zeros((6, width), F32)
    for n in range(chunks):
        b_in_sum = jnp.sum(r.sum_b_in[:, tile(n)], axis=0, keepdims=True)
        r.b_part[n] = jnp.concatenate([b_in_sum, b_out_sum, pad], axis=0)
    r.b_got[mine] = r.b_part[mine]
    b_first = []
    for i, (peer, at) in enumerate(zip(group, group_at)):
        copy = send(r.b_part.at[at], r.b_got.at[mine], r.b_sem, i, peer)
        copy.start()
        b_first.append(copy)

    depth = width
    parts = steps * rows // depth
    sources = ((r.xt, r.pre), (r.ut, r.act))

    def products(t, quarters):
        left_ref, right_ref = sources[t]
        for p in range(parts):
            k_rows = slice(p * depth, (p + 1) * depth)
            for u, n in zip(UNITS, quarters):
                lanes = pl.ds(pl.multiple_of(n * width, width), width)
                push(right_ref[k_rows, lanes], p % 2, u)
                multiply(wide[u], left_ref[:, k_rows], p % 2)
        return [pltpu.matmul_pop(wide[u]) for u in UNITS]

    near_copies = {}

    def exchange(t, i):
        away, keep = products(t, ((diagonal, across), (sibling, mine))[i])
        r.near_out[t, i] = away
        copy = send(r.near_out.at[t, i], r.near_in.at[t, i], r.grad_sem, 2 * t + i, to_sibling)
        copy.start()
        near_copies[t, i] = copy
        r.keep[t, i] = keep

    far_copies = []

    def cross(t):
        near_copies[t, 0].wait_recv()
        r.far_out[t] = (r.keep[t, 0] + r.near_in[t, 0]).astype(BF16)
        copy = send(r.far_out.at[t], r.far_in.at[t], r.cross_sem, t, to_across)
        copy.start()
        far_copies.append(copy)

    piece = width // members
    lane = r.scale.shape[3]
    scatter_copies = [[], []]

    def scatter(t):
        near_copies[t, 1].wait_recv()
        far_copies[t].wait_recv()
        full = r.keep[t, 1] + r.near_in[t, 1] + r.far_in[t].astype(F32)
        r.full[t] = full.reshape(members, piece, width)
        r.scatter_out[t] = full.astype(BF16).reshape(members, piece, width)
        for d, (peer, at) in enumerate(zip(others, others_at)):
            copy = send(
                r.scatter_out.at[t, at],
                r.scatter_in.at[t, d],
                r.scatter_sem,
                t * (members - 1) + d,
                peer,
            )
            copy.start()
            scatter_copies[t].append(copy)

    spread_copies = []

    def spread(t):
        value = r.full[t, batch]
        for d in range(members - 1):
            scatter_copies[t][d].wait_recv()
            value = value + r.scatter_in[t, d].astype(F32)
        value = value / total_rows
        top = jnp.max(jnp.abs(value), axis=0, keepdims=True)
        share = top[:, :lane]
        for m in range(1, width // lane):
            share = jnp.maximum(share, top[:, m * lane : (m + 1) * lane])
        scale = jnp.maximum(share, 1e-30) * (1.0 / 32767.0)
        grow = jnp.concatenate([1.0 / scale] * (width // lane), axis=1)
        r.done[t, batch] = jnp.round(value * grow).astype(jnp.int32).astype(jnp.int16)
        r.scale[t, batch] = scale
        for d, peer in enumerate(others):
            copy = send(
                r.scale.at[t, batch],
                r.scale.at[t, batch],
                r.scale_sem,
                t * (members - 1) + d,
                peer,
            )
            copy.start()
            spread_copies.append(copy)
        for d, peer in enumerate(others):
            copy = send(
                r.done.at[t, batch],
                r.done.at[t, batch],
                r.spread_sem,
                t * (members - 1) + d,
                peer,
            )
            copy.start()
            spread_copies.append(copy)

    def collect(t):
        for d, origin in enumerate(origins):
            for ref, sems in ((r.scale, r.scale_sem), (r.done, r.spread_sem)):
                at = ref.at[t, origin]
                send(at, at, sems, t * (members - 1) + d, (origin, mine)).wait_recv()

    exchange(0, 0)
    exchange(1, 0)
    cross(0)
    exchange(0, 1)
    cross(1)
    exchange(1, 1)
    for d, origin in enumerate(origins):
        send(
            r.dec_mid.at[origin], r.dec_mid.at[origin], r.dec_all_sem, d, (origin, mine)
        ).wait_recv()
    dec_total = r.dec_mid[0]
    for b in range(1, members):
        dec_total = dec_total + r.dec_mid[b]
    r.decs[mine] = dec_total / total_rows
    dec_third = []
    for i, peer in enumerate(group):
        copy = send(r.decs.at[mine], r.decs.at[mine], r.dec_out_sem, i, peer)
        copy.start()
        dec_third.append(copy)
    for i, (peer, at) in enumerate(zip(group, group_at)):
        send(r.b_part.at[at], r.b_got.at[at], r.b_sem, i, peer).wait_recv()
    b_sum = r.b_got[0]
    for n in range(1, chunks):
        b_sum = b_sum + r.b_got[n]
    r.b_mid[batch] = b_sum
    b_second = []
    for d, peer in enumerate(others):
        copy = send(r.b_mid.at[batch], r.b_mid.at[batch], r.b_all_sem, d, peer)
        copy.start()
        b_second.append(copy)
    scatter(0)
    scatter(1)
    spread(0)
    spread(1)
    for i, (peer, at) in enumerate(zip(group, group_at)):
        send(r.decs.at[at], r.decs.at[at], r.dec_out_sem, i, peer).wait_recv()
    for d, origin in enumerate(origins):
        send(
            r.b_mid.at[origin], r.b_mid.at[origin], r.b_all_sem, d, (origin, mine)
        ).wait_recv()
    b_total = r.b_mid[0]
    for b in range(1, members):
        b_total = b_total + r.b_mid[b]
    r.b_done[...] = b_total / total_rows
    for copy in (
        dec_first + dec_second + dec_third + b_first + b_second + list(near_copies.values()) + far_copies
    ):
        copy.wait_send()
    for copy in scatter_copies[0] + scatter_copies[1]:
        copy.wait_send()
    collect(0)
    collect(1)
    for copy in spread_copies:
        copy.wait_send()


def finish_kernel(
    done_ref,
    scale_ref,
    b_ref,
    decs_ref,
    cot_ref,
    elbo_ref,
    w_in_out,
    w_out_out,
    b_in_out,
    b_out_out,
    dec_out,
    scores_out,
    cot_out,
    elbo_out,
):
    _, members, piece, width = done_ref.shape
    lane = scale_ref.shape[3]

    def value(t, b):
        scale = jnp.concatenate([scale_ref[t, b]] * (width // lane), axis=1)
        return done_ref[t, b].astype(jnp.int32).astype(F32) * scale

    for b in range(members):
        part = slice(b * piece, (b + 1) * piece)
        w_in_out[part, :] = value(0, b)
    w_out_out[...] = jnp.concatenate([value(1, b) for b in range(members)], axis=0).T
    b_in_out[...] = b_ref[0:1, :]
    b_out_out[...] = b_ref[1:2, :]
    quarter = dec_out.shape[0] // decs_ref.shape[0]
    for n in range(decs_ref.shape[0]):
        dec_out[n * quarter : (n + 1) * quarter, :] = decs_ref[n, :quarter, :]
    likelihood = jnp.zeros((1, 1), F32)
    divergence = jnp.zeros((1, 1), F32)
    for n in range(decs_ref.shape[0]):
        share = decs_ref[n, quarter : quarter + 2, :]
        likelihood = share[0:1] if n == 0 else likelihood
        divergence = share[1:2] if n == 0 else divergence
    scores_out[:, 0:1] = jnp.sum(likelihood, axis=1, keepdims=True)
    scores_out[:, 1:2] = jnp.sum(divergence, axis=1, keepdims=True)
    cot_out[...] = cot_ref[...]
    elbo_out[...] = elbo_ref[...]


def on_device(
    init_state,
    brownian,
    step_size,
    lengths,
    obs_steps,
    observed,
    w_in,
    b_in,
    w_out,
    b_out,
    decoder,
    prior_rate,
    diffusion,
):
    rows, width = init_state.shape
    steps = brownian.shape[0]
    seen_count, seen_width = observed.shape[1:]
    chunks, members = lax.axis_size("mp"), lax.axis_size("batch")
    quarter = width // chunks
    piece = width // members
    total_rows = rows * chunks * members
    hidden = chunks * width
    hbm = pl.BlockSpec(memory_space=pltpu.HBM)
    vmem = pl.BlockSpec(memory_space=pltpu.VMEM)

    inputs = {
        "init_hbm": init_state,
        "noise_hbm": brownian,
        "step_hbm": step_size[None, :],
        "length_hbm": lengths[None, :],
        "obs_hbm": obs_steps.T,
        "seen_hbm": observed,
        "w_in_own": w_in,
        "b_in_own": b_in,
        "w_out_own": w_out,
        "b_out_hbm": b_out[None, :],
        "dec_hbm": decoder,
        "rate_hbm": prior_rate[None, :],
        "diff_hbm": diffusion[None, :],
    }
    outputs = {
        "done": ((2, members, piece, width), jnp.int16),
        "scale": ((2, members, 1, rows), F32),
        "b_done": ((8, width), F32),
        "decs": ((chunks, quarter + 8, seen_width), F32),
        "cot": ((rows, width), F32),
        "elbo": ((1, rows), F32),
    }
    scratch = {
        "init": ((rows, width), F32),
        "noise": ((steps, rows, width), BF16),
        "step": ((1, rows), F32),
        "length": ((1, rows), jnp.int32),
        "obs": ((seen_count, rows), jnp.int32),
        "seen": ((rows, seen_count, seen_width), BF16),
        "w_in": ((chunks, width, width), BF16),
        "w_out": ((chunks, width, width), BF16),
        "b_in_flat": ((width,), BF16),
        "bias_own": ((8, width), F32),
        "bias": ((chunks, 8, width), F32),
        "bias_row": ((1, hidden), F32),
        "b_out": ((1, width), F32),
        "dec": ((width, seen_width), BF16),
        "rate": ((1, width), F32),
        "diff": ((1, width), F32),
        "w_in_t": ((chunks, width, width), BF16),
        "w_out_t": ((chunks, width, width), BF16),
        "dec_wide": ((width, width), BF16),
        "dec_t": ((2 * seen_width, width), BF16),
        "dt": ((rows, rows), F32),
        "root": ((rows, rows), F32),
        "len_wide": ((rows, rows), jnp.int32),
        "obs_wide": ((seen_count, rows, rows), jnp.int32),
        "obs_half": ((seen_count, rows, rows), jnp.int16),
        "picked": ((seen_count, rows, width), BF16),
        "misfit": ((seen_count, rows, seen_width), F32),
        "misfit_wide": ((seen_count * rows, width), BF16),
        "target": ((rows * seen_count, seen_width), F32),
        "state": ((rows, width), F32),
        "kl": ((rows, width), F32),
        "sum_b_in": ((8, hidden), F32),
        "sum_b_out": ((8, width), F32),
        "x": ((steps + 1, rows, width), BF16),
        "xt": ((width, steps * rows), BF16),
        "ut": ((width, steps * rows), BF16),
        "act": ((steps * rows, hidden), BF16),
        "pre": ((steps * rows, hidden), BF16),
        "scaled": ((steps, rows, width), F32),
        "dec_part": ((chunks, quarter + 8, seen_width), F32),
        "dec_got": ((3, quarter + 8, seen_width), F32),
        "dec_mid": ((members, quarter + 8, seen_width), F32),
        "b_part": ((chunks, 8, width), F32),
        "b_got": ((chunks, 8, width), F32),
        "b_mid": ((members, 8, width), F32),
        "near_out": ((2, 2, width, width), F32),
        "near_in": ((2, 2, width, width), F32),
        "keep": ((2, 2, width, width), F32),
        "far_out": ((2, width, width), BF16),
        "far_in": ((2, width, width), BF16),
        "full": ((2, members, piece, width), F32),
        "scatter_out": ((2, members, piece, width), BF16),
        "scatter_in": ((2, members - 1, piece, width), BF16),
    }
    waits = {
        "far_sem": 3,
        "near_sem": 3,
        "relay_sem": 3,
        "dec_sem": 3,
        "dec_all_sem": members - 1,
        "dec_out_sem": 3,
        "b_sem": 3,
        "b_all_sem": members - 1,
        "grad_sem": 4,
        "cross_sem": 2,
        "scatter_sem": 2 * (members - 1),
        "spread_sem": 2 * (members - 1),
        "scale_sem": 2 * (members - 1),
    }

    def body(*refs):
        refs = list(refs)
        named = Refs(
            list(inputs) + list(outputs) + list(scratch),
            refs[: len(inputs) + len(outputs) + len(scratch)],
        )
        sems = refs[len(inputs) + len(outputs) + len(scratch) :]
        named.load_sem = sems.pop(0)
        for name in waits:
            setattr(named, name, (sems.pop(0), sems.pop(0)))

        def with_accs(*accs):
            named.first, named.second, named.third = accs[0:2], accs[2:4], accs[4:6]
            named.wide, named.aside = accs[6:8], accs[8]
            train_kernel(named, members, total_rows)

        pl.run_scoped(
            with_accs,
            *[pltpu.ACC(u)((rows, width), F32) for _ in range(3) for u in UNITS],
            *[pltpu.ACC(u)((width, width), F32) for u in UNITS],
            pltpu.ACC(0)((rows, width), F32),
        )

    sem_shapes = [pltpu.SemaphoreType.DMA((len(inputs),))]
    for count in waits.values():
        sem_shapes += [pltpu.SemaphoreType.DMA((count,))] * 2
    done, scale, b_done, decs, cot, elbo = pl.pallas_call(
        body,
        out_shape=[jax.ShapeDtypeStruct(*s) for s in outputs.values()],
        in_specs=[hbm] * len(inputs),
        out_specs=[vmem] * len(outputs),
        scratch_shapes=[pltpu.VMEM(*s) for s in scratch.values()] + sem_shapes,
        compiler_params=pltpu.CompilerParams(
            collective_id=0, has_side_effects=True, vmem_limit_bytes=LIMIT
        ),
        name="train",
    )(*[pltpu.with_memory_space_constraint(v, pltpu.HBM) for v in inputs.values()])
    results = pl.pallas_call(
        finish_kernel,
        out_shape=[
            jax.ShapeDtypeStruct((width, width), F32),
            jax.ShapeDtypeStruct((width, width), F32),
            jax.ShapeDtypeStruct((1, width), F32),
            jax.ShapeDtypeStruct((1, width), F32),
            jax.ShapeDtypeStruct((width, seen_width), F32),
            jax.ShapeDtypeStruct((1, 2), F32),
            jax.ShapeDtypeStruct((rows, width), F32),
            jax.ShapeDtypeStruct((1, rows), F32),
        ],
        in_specs=[vmem] * 6,
        out_specs=[vmem] * 8,
        compiler_params=pltpu.CompilerParams(vmem_limit_bytes=4 * 1024 * 1024),
        name="finish",
    )(done, scale, b_done, decs, cot, elbo)
    own_w_in, own_w_out, own_b_in, b_out_grad, dec_grad, scores, grad_init, elbo = results
    return (
        elbo[0],
        scores[0],
        own_w_in,
        own_b_in[0],
        own_w_out,
        b_out_grad[0],
        dec_grad,
        grad_init,
    )


def solution(mesh):
    both = ("batch", "mp")
    placed = (
        P(both, None),
        P(None, both, None),
        P(both),
        P(both),
        P(both, None),
        P(both, None, None),
        P(None, "mp"),
        P("mp"),
        P("mp", None),
        P(),
        P(),
        P(),
        P(),
    )
    return jax.shard_map(
        on_device,
        mesh=mesh,
        in_specs=placed,
        out_specs=(
            P(both),
            P(),
            P(None, "mp"),
            P("mp"),
            P("mp", None),
            P(),
            P(),
            P(both, None),
        ),
        check_vma=False,
    )
```

```python
import jax
import jax.numpy as jnp
from jax import lax
from jax.experimental import pallas as pl
from jax.experimental.pallas import tpu as pltpu
from jax.sharding import PartitionSpec as P

F32 = jnp.float32
BF16 = jnp.bfloat16
UNITS = (0, 1)
UNROLL = 2
LIMIT = 48 * 1024 * 1024


def fold(value):
    return value.reshape(-1, 8, value.shape[1]).sum(axis=0)


def send(source, target, sems, index, peer):
    return pltpu.make_async_remote_copy(
        src_ref=source,
        dst_ref=target,
        send_sem=sems[0].at[index],
        recv_sem=sems[1].at[index],
        device_id=peer,
        device_id_type=pl.DeviceIdType.MESH,
    )


def push(value, slot, unit):
    pltpu.matmul_push_rhs(value, slot, unit)


def multiply(acc, value, slot):
    pltpu.matmul_acc_lhs(acc, value, load_staged_rhs=slot)


class Refs:
    def __init__(self, names, refs):
        for name, ref in zip(names, refs, strict=True):
            setattr(self, name, ref)


def train_kernel(r, members, total_rows):
    rows, width = r.init.shape
    steps = r.noise.shape[0]
    seen_count = r.obs.shape[0]
    seen_width = r.dec.shape[1]
    chunks = r.w_in.shape[0]
    first, second, third, aside, wide = r.first, r.second, r.third, r.aside, r.wide

    mine = lax.axis_index("mp")
    batch = lax.axis_index("batch")
    chip, unit = mine // 2, mine % 2
    sibling = chip * 2 + (1 - unit)
    across = (1 - chip) * 2 + unit
    diagonal = (1 - chip) * 2 + (1 - unit)
    to_sibling, to_across, to_diagonal = (batch, sibling), (batch, across), (batch, diagonal)
    group = (to_sibling, to_across, to_diagonal)
    group_at = (sibling, across, diagonal)
    order = sorted(range(1, members), key=lambda d: abs(d - members // 2))
    others_at = [lax.rem(batch + d, members) for d in order]
    others = [(at, mine) for at in others_at]
    origins = [lax.rem(batch + members - d, members) for d in order]

    loads = {}
    for i, (name, source, target) in enumerate(
        (
            ("w_in", r.w_in_own, r.w_in.at[mine]),
            ("b_in", r.b_in_own, r.b_in_flat),
            ("w_out", r.w_out_own, r.w_out.at[mine]),
            ("step", r.step_hbm, r.step),
            ("length", r.length_hbm, r.length),
            ("obs", r.obs_hbm, r.obs),
            ("init", r.init_hbm, r.init),
            ("b_out", r.b_out_hbm, r.b_out),
            ("dec", r.dec_hbm, r.dec),
            ("rate", r.rate_hbm, r.rate),
            ("diff", r.diff_hbm, r.diff),
            ("noise", r.noise_hbm, r.noise),
            ("seen", r.seen_hbm, r.seen),
        )
    ):
        loads[name] = pltpu.make_async_copy(source, target, r.load_sem.at[i])
        loads[name].start()

    barrier = pltpu.get_barrier_semaphore()
    for peer in list(group) + others:
        pl.semaphore_signal(barrier, inc=1, device_id=peer, device_id_type=pl.DeviceIdType.MESH)
    loads["b_in"].wait()
    r.bias_own[...] = jnp.broadcast_to(
        r.b_in_flat[...].astype(F32).reshape(1, width), r.bias_own.shape
    )
    pl.semaphore_wait(barrier, len(group) + len(others))

    whole = (r.w_in, r.bias, r.w_out)
    own = (r.w_in.at[mine], r.bias_own, r.w_out.at[mine])
    loads["w_in"].wait()
    far, near = [None] * 3, [None] * 3
    for i in (0, 1, 2):
        if i == 2:
            loads["w_out"].wait()
        far[i] = send(own[i], whole[i].at[mine], r.far_sem, i, to_across)
        far[i].start()
        near[i] = send(own[i], whole[i].at[mine], r.near_sem, i, to_sibling)
        near[i].start()
    r.bias[mine] = r.bias_own[...]

    def column(row):
        return jnp.broadcast_to(row, (rows, rows)).T

    for name in ("step", "length", "obs", "init", "b_out", "dec", "rate", "diff"):
        loads[name].wait()
    r.dt[...] = column(r.step[...])
    r.root[...] = jnp.sqrt(r.dt[...])
    r.len_wide[...] = column(r.length[...])
    for j in range(seen_count):
        wide_obs = column(r.obs[j : j + 1, :])
        r.obs_wide[j] = wide_obs
        r.obs_half[j] = wide_obs.astype(jnp.int16)
    r.kl[...] = jnp.zeros_like(r.kl)
    r.sum_b_in[...] = jnp.zeros_like(r.sum_b_in)
    r.sum_b_out[...] = jnp.zeros_like(r.sum_b_out)
    r.state[...] = r.init[...]
    r.x[0] = r.init[...].astype(BF16)
    r.dec_wide[:, :seen_width] = r.dec[...]
    r.dec_wide[:, seen_width:] = jnp.zeros((width, width - seen_width), BF16)
    dec_t = r.dec[...].T
    r.dec_t[:seen_width, :] = dec_t
    r.dec_t[seen_width:, :] = dec_t
    for u in UNITS:
        for acc in (first[u], second[u], third[u], wide[u]):
            pltpu.matmul_pop(acc)
    pltpu.matmul_pop(aside)

    relayed = []
    for i in (0, 1, 2):
        far[i].wait_recv()
        at = whole[i].at[across]
        copy = send(at, at, r.relay_sem, i, to_sibling)
        copy.start()
        relayed.append(copy)
    loads["noise"].wait()
    loads["seen"].wait()
    r.target[...] = r.seen[...].astype(F32).reshape(r.target.shape)
    for copy in far:
        copy.wait_send()
    for copy in near + relayed:
        copy.wait()

    pair = len(UNITS)
    halves = chunks // pair

    def tile(n):
        return slice(n * width, (n + 1) * width)

    def both(value):
        return jnp.concatenate([value] * (width // rows), axis=1)

    for n in range(chunks):
        r.bias_row[:, tile(n)] = r.bias[n, :1, :]

    def stage_pair(read):
        for slot in range(halves):
            for u in UNITS:
                push(read(slot * pair + u), slot, u)

    def discharge():
        for u in UNITS:
            for slot, acc in ((0, first[u]), (1, second[u])):
                multiply(acc, r.x[0], slot)
                pltpu.matmul_pop(acc)

    def two_phases(x, side, between, later, upcoming):
        for u in UNITS:
            multiply(first[u], x, 0)
        if side is not None:
            push(side[1], 0, 0)
            push(later(1), 0, 1)
        else:
            for u in UNITS:
                push(later(u), 0, u)
        for u in UNITS:
            multiply(second[u], x, 1)
        for u in UNITS:
            push(later(pair + u), 1, u)
        if side is not None:
            multiply(aside, side[0], 0)
            push(later(0), 0, 0)
        for u in UNITS:
            multiply(third[u], between(u, pltpu.matmul_pop(first[u])), 0)
        for u in UNITS:
            push(upcoming(u), 0, u)
        for u in UNITS:
            multiply(third[u], between(pair + u, pltpu.matmul_pop(second[u])), 1)
        for u in UNITS:
            push(upcoming(pair + u), 1, u)
        extra = pltpu.matmul_pop(aside) if side is not None else None
        return pltpu.matmul_pop(third[0]) + pltpu.matmul_pop(third[1]), extra

    band = 16

    def pick_band(b, carry):
        at = pl.ds(pl.multiple_of(b * band, band), band)
        wanted = [r.obs_half[j, at, :] for j in range(seen_count)]

        def look(k, found):
            x = r.x[k, at, :]
            index = jnp.full((band, rows), k, jnp.int32).astype(jnp.int16)
            out = []
            for j in range(seen_count):
                hit = wanted[j] == index
                for m in range(width // rows):
                    at_m = j * (width // rows) + m
                    out.append(jnp.where(hit, x[:, m * rows : (m + 1) * rows], found[at_m]))
            return tuple(out)

        blank = jnp.zeros((band, rows), BF16)
        found = lax.fori_loop(
            1, steps + 1, look, (blank,) * (seen_count * (width // rows)), unroll=4
        )
        for j in range(seen_count):
            for m in range(width // rows):
                r.picked[j, at, m * rows : (m + 1) * rows] = found[j * (width // rows) + m]
        return carry

    def forward(k, carry):
        x = r.x[k]

        def between(n, raw):
            act = jnp.tanh(raw + r.bias_row[:, tile(n)]).astype(BF16)
            r.act[pl.ds(k * rows, rows), tile(n)] = act
            return act

        total, _ = two_phases(x, None, between, lambda n: r.w_out[n], lambda n: r.w_in[n])
        drift = total + r.b_out[...]
        state = r.state[...]
        inv = 1.0 / r.diff[...]
        live = k < r.len_wide[...]
        factor = both(jnp.where(live, r.dt[...], 0.0))
        root = both(jnp.where(live, r.root[...], 0.0))
        following = state + (factor * drift + r.diff[...] * root * r.noise[k].astype(F32))
        r.state[...] = following
        r.x[k + 1] = following.astype(BF16)
        residual = (drift + r.rate[...] * state) * inv
        r.kl[...] += factor * residual * residual
        r.scaled[k] = residual * inv
        r.xt[:, pl.ds(pl.multiple_of(k * rows, rows), rows)] = x.T
        return carry

    stage_pair(lambda n: r.w_in[n])
    lax.fori_loop(0, steps, forward, 0, unroll=UNROLL)
    discharge()
    lax.fori_loop(0, rows // band, pick_band, 0)

    square = jnp.zeros((rows, seen_width), F32)
    seen_accs = (first[0], first[1], second[0], second[1])
    for u in UNITS:
        push(r.dec_wide[...], 0, u)
    loaded = [False, False]
    for start in range(0, seen_count, len(seen_accs)):
        batch_j = list(range(start, min(start + len(seen_accs), seen_count)))
        for at, (acc, j) in enumerate(zip(seen_accs, batch_j)):
            u = at % 2
            multiply(acc, r.picked[j], None if loaded[u] else 0)
            loaded[u] = True
        for acc, j in zip(seen_accs, batch_j):
            misfit = (
                pltpu.matmul_pop(acc)[:, :seen_width]
                - r.target[pl.ds(j, rows, stride=seen_count), :]
            )
            square = square + misfit * misfit
            rounded = misfit.astype(BF16)
            r.misfit[j] = rounded.astype(F32)
            r.misfit_wide[j * rows : (j + 1) * rows, :seen_width] = rounded
    r.misfit_wide[:, seen_width:] = jnp.zeros(
        (seen_count * rows, width - seen_width), BF16
    )
    per = width // rows
    for p in range(seen_count // per):
        u = p % 2
        left = jnp.concatenate([r.picked[p * per + m].T for m in range(per)], axis=1)
        push(r.misfit_wide[p * width : (p + 1) * width, :], 0, u)
        multiply(wide[u], left, 0)
    dec_grad = (pltpu.matmul_pop(wide[0]) + pltpu.matmul_pop(wide[1]))[:, :seen_width]
    loglik = -0.5 * jnp.sum(square.T, axis=0, keepdims=True)
    kl_half = r.kl[:, :rows]
    for part in range(1, width // rows):
        kl_half = kl_half + r.kl[:, part * rows : (part + 1) * rows]
    kl_row = 0.5 * jnp.sum(kl_half.T, axis=0, keepdims=True)
    divisor = (width * r.length[...] + seen_width * seen_count).astype(F32)
    r.elbo[...] = (loglik - kl_row) / divisor

    quarter = width // chunks
    score_rows = jnp.concatenate(
        [loglik, kl_row, jnp.zeros((6, rows), F32)], axis=0
    )
    for n in range(chunks):
        r.dec_part[n, :quarter, :] = dec_grad[n * quarter : (n + 1) * quarter, :]
        r.dec_part[n, quarter:, :] = score_rows
    dec_first = []
    for i, (peer, at) in enumerate(zip(group, group_at)):
        copy = send(r.dec_part.at[at], r.dec_got.at[i], r.dec_sem, i, peer)
        copy.start()
        dec_first.append(copy)

    for n in range(chunks):
        r.w_in_t[n] = r.w_in[n].T
        r.w_out_t[n] = r.w_out[n].T

    def obs_sum(index):
        total = jnp.zeros((rows, seen_width), F32)
        for j in range(seen_count):
            total = total + jnp.where(r.obs_wide[j] == index, r.misfit[j], 0.0)
        high = total.astype(BF16)
        low = (total - high.astype(F32)).astype(BF16)
        return jnp.concatenate([high, low], axis=1)

    push(r.dec_t[...], 0, 0)
    multiply(aside, obs_sum(steps), 0)
    r.cot[...] = pltpu.matmul_pop(aside)
    stage_pair(lambda n: r.w_out_t[n])

    def backward(index, carry):
        k = steps - 1 - index
        cot = r.cot[...]
        scaled = r.scaled[k]
        factor = both(jnp.where(k < r.len_wide[...], r.dt[...], 0.0))
        update = factor * (cot + scaled)
        rounded = update.astype(BF16)

        def between(n, raw):
            act = r.act[pl.ds(k * rows, rows), tile(n)].astype(F32)
            pre = raw * (1.0 - act * act)
            pre_round = pre.astype(BF16)
            r.pre[pl.ds(k * rows, rows), tile(n)] = pre_round
            r.sum_b_in[:, tile(n)] += fold(pre)
            return pre_round

        total, seen_back = two_phases(
            rounded,
            (obs_sum(k), r.dec_t[...]),
            between,
            lambda n: r.w_in_t[n],
            lambda n: r.w_out_t[n],
        )
        r.cot[...] = total + (cot + factor * r.rate[...] * scaled + seen_back)
        r.ut[:, pl.ds(pl.multiple_of(k * rows, rows), rows)] = rounded.T
        r.sum_b_out[...] += fold(update)
        return carry

    cut = steps * 3 // 8 // 2 * 2
    lax.fori_loop(0, cut, backward, 0, unroll=UNROLL)
    for copy in dec_first:
        copy.wait_recv()
    dec_sum = r.dec_part[mine]
    for i in range(len(group)):
        dec_sum = dec_sum + r.dec_got[i]
    r.dec_mid[batch] = dec_sum
    dec_second = []
    for d, peer in enumerate(others):
        copy = send(r.dec_mid.at[batch], r.dec_mid.at[batch], r.dec_all_sem, d, peer)
        copy.start()
        dec_second.append(copy)
    lax.fori_loop(cut, steps, backward, 0, unroll=UNROLL)
    discharge()

    b_out_sum = jnp.sum(r.sum_b_out[...], axis=0, keepdims=True)
    pad = jnp.zeros((6, width), F32)
    for n in range(chunks):
        b_in_sum = jnp.sum(r.sum_b_in[:, tile(n)], axis=0, keepdims=True)
        r.b_part[n] = jnp.concatenate([b_in_sum, b_out_sum, pad], axis=0)
    r.b_got[mine] = r.b_part[mine]
    b_first = []
    for i, (peer, at) in enumerate(zip(group, group_at)):
        copy = send(r.b_part.at[at], r.b_got.at[mine], r.b_sem, i, peer)
        copy.start()
        b_first.append(copy)

    depth = width
    parts = steps * rows // depth
    sources = ((r.xt, r.pre), (r.ut, r.act))

    def products(t, quarters):
        left_ref, right_ref = sources[t]
        for p in range(parts):
            k_rows = slice(p * depth, (p + 1) * depth)
            for u, n in zip(UNITS, quarters):
                lanes = pl.ds(pl.multiple_of(n * width, width), width)
                push(right_ref[k_rows, lanes], p % 2, u)
                multiply(wide[u], left_ref[:, k_rows], p % 2)
        return [pltpu.matmul_pop(wide[u]) for u in UNITS]

    near_copies = {}

    def exchange(t, i):
        away, keep = products(t, ((diagonal, across), (sibling, mine))[i])
        r.near_out[t, i] = away
        copy = send(r.near_out.at[t, i], r.near_in.at[t, i], r.grad_sem, 2 * t + i, to_sibling)
        copy.start()
        near_copies[t, i] = copy
        r.keep[t, i] = keep

    far_copies = []

    def cross(t):
        near_copies[t, 0].wait_recv()
        r.far_out[t] = (r.keep[t, 0] + r.near_in[t, 0]).astype(BF16)
        copy = send(r.far_out.at[t], r.far_in.at[t], r.cross_sem, t, to_across)
        copy.start()
        far_copies.append(copy)

    piece = width // members
    lane = r.scale.shape[3]
    scatter_copies = [[], []]

    def scatter(t):
        near_copies[t, 1].wait_recv()
        far_copies[t].wait_recv()
        full = r.keep[t, 1] + r.near_in[t, 1] + r.far_in[t].astype(F32)
        r.full[t] = full.reshape(members, piece, width)
        r.scatter_out[t] = full.astype(BF16).reshape(members, piece, width)
        for d, (peer, at) in enumerate(zip(others, others_at)):
            copy = send(
                r.scatter_out.at[t, at],
                r.scatter_in.at[t, d],
                r.scatter_sem,
                t * (members - 1) + d,
                peer,
            )
            copy.start()
            scatter_copies[t].append(copy)

    spread_copies = []

    def spread(t):
        value = r.full[t, batch]
        for d in range(members - 1):
            scatter_copies[t][d].wait_recv()
            value = value + r.scatter_in[t, d].astype(F32)
        value = value / total_rows
        top = jnp.max(jnp.abs(value), axis=0, keepdims=True)
        share = top[:, :lane]
        for m in range(1, width // lane):
            share = jnp.maximum(share, top[:, m * lane : (m + 1) * lane])
        scale = jnp.maximum(share, 1e-30) * (1.0 / 32767.0)
        grow = jnp.concatenate([1.0 / scale] * (width // lane), axis=1)
        r.done[t, batch] = jnp.round(value * grow).astype(jnp.int32).astype(jnp.int16)
        r.scale[t, batch] = scale
        for d, peer in enumerate(others):
            copy = send(
                r.scale.at[t, batch],
                r.scale.at[t, batch],
                r.scale_sem,
                t * (members - 1) + d,
                peer,
            )
            copy.start()
            spread_copies.append(copy)
        for d, peer in enumerate(others):
            copy = send(
                r.done.at[t, batch],
                r.done.at[t, batch],
                r.spread_sem,
                t * (members - 1) + d,
                peer,
            )
            copy.start()
            spread_copies.append(copy)

    def collect(t):
        for d, origin in enumerate(origins):
            for ref, sems in ((r.scale, r.scale_sem), (r.done, r.spread_sem)):
                at = ref.at[t, origin]
                send(at, at, sems, t * (members - 1) + d, (origin, mine)).wait_recv()

    exchange(0, 0)
    exchange(1, 0)
    cross(0)
    exchange(0, 1)
    cross(1)
    exchange(1, 1)
    for d, origin in enumerate(origins):
        send(
            r.dec_mid.at[origin], r.dec_mid.at[origin], r.dec_all_sem, d, (origin, mine)
        ).wait_recv()
    dec_total = r.dec_mid[0]
    for b in range(1, members):
        dec_total = dec_total + r.dec_mid[b]
    r.decs[mine] = dec_total / total_rows
    dec_third = []
    for i, peer in enumerate(group):
        copy = send(r.decs.at[mine], r.decs.at[mine], r.dec_out_sem, i, peer)
        copy.start()
        dec_third.append(copy)
    for i, (peer, at) in enumerate(zip(group, group_at)):
        send(r.b_part.at[at], r.b_got.at[at], r.b_sem, i, peer).wait_recv()
    b_sum = r.b_got[0]
    for n in range(1, chunks):
        b_sum = b_sum + r.b_got[n]
    r.b_mid[batch] = b_sum
    b_second = []
    for d, peer in enumerate(others):
        copy = send(r.b_mid.at[batch], r.b_mid.at[batch], r.b_all_sem, d, peer)
        copy.start()
        b_second.append(copy)
    scatter(0)
    scatter(1)
    spread(0)
    spread(1)
    for i, (peer, at) in enumerate(zip(group, group_at)):
        send(r.decs.at[at], r.decs.at[at], r.dec_out_sem, i, peer).wait_recv()
    for d, origin in enumerate(origins):
        send(
            r.b_mid.at[origin], r.b_mid.at[origin], r.b_all_sem, d, (origin, mine)
        ).wait_recv()
    b_total = r.b_mid[0]
    for b in range(1, members):
        b_total = b_total + r.b_mid[b]
    r.b_done[...] = b_total / total_rows
    for copy in (
        dec_first + dec_second + dec_third + b_first + b_second + list(near_copies.values()) + far_copies
    ):
        copy.wait_send()
    for copy in scatter_copies[0] + scatter_copies[1]:
        copy.wait_send()
    collect(0)
    collect(1)
    for copy in spread_copies:
        copy.wait_send()


def finish_kernel(
    done_ref,
    scale_ref,
    b_ref,
    decs_ref,
    cot_ref,
    elbo_ref,
    w_in_out,
    w_out_out,
    b_in_out,
    b_out_out,
    dec_out,
    scores_out,
    cot_out,
    elbo_out,
):
    _, members, piece, width = done_ref.shape
    lane = scale_ref.shape[3]

    def value(t, b):
        scale = jnp.concatenate([scale_ref[t, b]] * (width // lane), axis=1)
        return done_ref[t, b].astype(jnp.int32).astype(F32) * scale

    for b in range(members):
        part = slice(b * piece, (b + 1) * piece)
        w_in_out[part, :] = value(0, b)
    w_out_out[...] = jnp.concatenate([value(1, b) for b in range(members)], axis=0).T
    b_in_out[...] = b_ref[0:1, :]
    b_out_out[...] = b_ref[1:2, :]
    quarter = dec_out.shape[0] // decs_ref.shape[0]
    for n in range(decs_ref.shape[0]):
        dec_out[n * quarter : (n + 1) * quarter, :] = decs_ref[n, :quarter, :]
    likelihood = jnp.zeros((1, 1), F32)
    divergence = jnp.zeros((1, 1), F32)
    for n in range(decs_ref.shape[0]):
        share = decs_ref[n, quarter : quarter + 2, :]
        likelihood = share[0:1] if n == 0 else likelihood
        divergence = share[1:2] if n == 0 else divergence
    scores_out[:, 0:1] = jnp.sum(likelihood, axis=1, keepdims=True)
    scores_out[:, 1:2] = jnp.sum(divergence, axis=1, keepdims=True)
    cot_out[...] = cot_ref[...]
    elbo_out[...] = elbo_ref[...]


def on_device(
    init_state,
    brownian,
    step_size,
    lengths,
    obs_steps,
    observed,
    w_in,
    b_in,
    w_out,
    b_out,
    decoder,
    prior_rate,
    diffusion,
):
    rows, width = init_state.shape
    steps = brownian.shape[0]
    seen_count, seen_width = observed.shape[1:]
    chunks, members = lax.axis_size("mp"), lax.axis_size("batch")
    quarter = width // chunks
    piece = width // members
    total_rows = rows * chunks * members
    hidden = chunks * width
    hbm = pl.BlockSpec(memory_space=pltpu.HBM)
    vmem = pl.BlockSpec(memory_space=pltpu.VMEM)

    inputs = {
        "init_hbm": init_state,
        "noise_hbm": brownian,
        "step_hbm": step_size[None, :],
        "length_hbm": lengths[None, :],
        "obs_hbm": obs_steps.T,
        "seen_hbm": observed,
        "w_in_own": w_in,
        "b_in_own": b_in,
        "w_out_own": w_out,
        "b_out_hbm": b_out[None, :],
        "dec_hbm": decoder,
        "rate_hbm": prior_rate[None, :],
        "diff_hbm": diffusion[None, :],
    }
    outputs = {
        "done": ((2, members, piece, width), jnp.int16),
        "scale": ((2, members, 1, rows), F32),
        "b_done": ((8, width), F32),
        "decs": ((chunks, quarter + 8, seen_width), F32),
        "cot": ((rows, width), F32),
        "elbo": ((1, rows), F32),
    }
    scratch = {
        "init": ((rows, width), F32),
        "noise": ((steps, rows, width), BF16),
        "step": ((1, rows), F32),
        "length": ((1, rows), jnp.int32),
        "obs": ((seen_count, rows), jnp.int32),
        "seen": ((rows, seen_count, seen_width), BF16),
        "w_in": ((chunks, width, width), BF16),
        "w_out": ((chunks, width, width), BF16),
        "b_in_flat": ((width,), BF16),
        "bias_own": ((8, width), F32),
        "bias": ((chunks, 8, width), F32),
        "bias_row": ((1, hidden), F32),
        "b_out": ((1, width), F32),
        "dec": ((width, seen_width), BF16),
        "rate": ((1, width), F32),
        "diff": ((1, width), F32),
        "w_in_t": ((chunks, width, width), BF16),
        "w_out_t": ((chunks, width, width), BF16),
        "dec_wide": ((width, width), BF16),
        "dec_t": ((2 * seen_width, width), BF16),
        "dt": ((rows, rows), F32),
        "root": ((rows, rows), F32),
        "len_wide": ((rows, rows), jnp.int32),
        "obs_wide": ((seen_count, rows, rows), jnp.int32),
        "obs_half": ((seen_count, rows, rows), jnp.int16),
        "picked": ((seen_count, rows, width), BF16),
        "misfit": ((seen_count, rows, seen_width), F32),
        "misfit_wide": ((seen_count * rows, width), BF16),
        "target": ((rows * seen_count, seen_width), F32),
        "state": ((rows, width), F32),
        "kl": ((rows, width), F32),
        "sum_b_in": ((8, hidden), F32),
        "sum_b_out": ((8, width), F32),
        "x": ((steps + 1, rows, width), BF16),
        "xt": ((width, steps * rows), BF16),
        "ut": ((width, steps * rows), BF16),
        "act": ((steps * rows, hidden), BF16),
        "pre": ((steps * rows, hidden), BF16),
        "scaled": ((steps, rows, width), F32),
        "dec_part": ((chunks, quarter + 8, seen_width), F32),
        "dec_got": ((3, quarter + 8, seen_width), F32),
        "dec_mid": ((members, quarter + 8, seen_width), F32),
        "b_part": ((chunks, 8, width), F32),
        "b_got": ((chunks, 8, width), F32),
        "b_mid": ((members, 8, width), F32),
        "near_out": ((2, 2, width, width), F32),
        "near_in": ((2, 2, width, width), F32),
        "keep": ((2, 2, width, width), F32),
        "far_out": ((2, width, width), BF16),
        "far_in": ((2, width, width), BF16),
        "full": ((2, members, piece, width), F32),
        "scatter_out": ((2, members, piece, width), BF16),
        "scatter_in": ((2, members - 1, piece, width), BF16),
    }
    waits = {
        "far_sem": 3,
        "near_sem": 3,
        "relay_sem": 3,
        "dec_sem": 3,
        "dec_all_sem": members - 1,
        "dec_out_sem": 3,
        "b_sem": 3,
        "b_all_sem": members - 1,
        "grad_sem": 4,
        "cross_sem": 2,
        "scatter_sem": 2 * (members - 1),
        "spread_sem": 2 * (members - 1),
        "scale_sem": 2 * (members - 1),
    }

    def body(*refs):
        refs = list(refs)
        named = Refs(
            list(inputs) + list(outputs) + list(scratch),
            refs[: len(inputs) + len(outputs) + len(scratch)],
        )
        sems = refs[len(inputs) + len(outputs) + len(scratch) :]
        named.load_sem = sems.pop(0)
        for name in waits:
            setattr(named, name, (sems.pop(0), sems.pop(0)))

        def with_accs(*accs):
            named.first, named.second, named.third = accs[0:2], accs[2:4], accs[4:6]
            named.wide, named.aside = accs[6:8], accs[8]
            train_kernel(named, members, total_rows)

        pl.run_scoped(
            with_accs,
            *[pltpu.ACC(u)((rows, width), F32) for _ in range(3) for u in UNITS],
            *[pltpu.ACC(u)((width, width), F32) for u in UNITS],
            pltpu.ACC(0)((rows, width), F32),
        )

    sem_shapes = [pltpu.SemaphoreType.DMA((len(inputs),))]
    for count in waits.values():
        sem_shapes += [pltpu.SemaphoreType.DMA((count,))] * 2
    done, scale, b_done, decs, cot, elbo = pl.pallas_call(
        body,
        out_shape=[jax.ShapeDtypeStruct(*s) for s in outputs.values()],
        in_specs=[hbm] * len(inputs),
        out_specs=[vmem] * len(outputs),
        scratch_shapes=[pltpu.VMEM(*s) for s in scratch.values()] + sem_shapes,
        compiler_params=pltpu.CompilerParams(
            collective_id=0, has_side_effects=True, vmem_limit_bytes=LIMIT
        ),
        name="train",
    )(*[pltpu.with_memory_space_constraint(v, pltpu.HBM) for v in inputs.values()])
    results = pl.pallas_call(
        finish_kernel,
        out_shape=[
            jax.ShapeDtypeStruct((width, width), F32),
            jax.ShapeDtypeStruct((width, width), F32),
            jax.ShapeDtypeStruct((1, width), F32),
            jax.ShapeDtypeStruct((1, width), F32),
            jax.ShapeDtypeStruct((width, seen_width), F32),
            jax.ShapeDtypeStruct((1, 2), F32),
            jax.ShapeDtypeStruct((rows, width), F32),
            jax.ShapeDtypeStruct((1, rows), F32),
        ],
        in_specs=[vmem] * 6,
        out_specs=[vmem] * 8,
        compiler_params=pltpu.CompilerParams(vmem_limit_bytes=4 * 1024 * 1024),
        name="finish",
    )(done, scale, b_done, decs, cot, elbo)
    own_w_in, own_w_out, own_b_in, b_out_grad, dec_grad, scores, grad_init, elbo = results
    return (
        elbo[0],
        scores[0],
        own_w_in,
        own_b_in[0],
        own_w_out,
        b_out_grad[0],
        dec_grad,
        grad_init,
    )


def solution(mesh):
    both = ("batch", "mp")
    placed = (
        P(both, None),
        P(None, both, None),
        P(both),
        P(both),
        P(both, None),
        P(both, None, None),
        P(None, "mp"),
        P("mp"),
        P("mp", None),
        P(),
        P(),
        P(),
        P(),
    )
    return jax.shard_map(
        on_device,
        mesh=mesh,
        in_specs=placed,
        out_specs=(
            P(both),
            P(),
            P(None, "mp"),
            P("mp"),
            P("mp", None),
            P(),
            P(),
            P(both, None),
        ),
        check_vma=False,
    )
```
